16 devices in a mesh: dp: 2 (over y, z), sp: 8 (over x, core).
Axes of the slice: x: 4, y: 2, z: 1, core: 2. Of those that a mesh axis runs over, the one named last changes fastest.
The devices are a block of a 4x4x8 slice.
Arguments:
- x: bfloat16 [4096, 4096], P(('dp', 'sp')), parts along dimension 0
- gain: bfloat16 [4096], replicated
- wq: bfloat16 [4096, 6144], replicated
- wk: bfloat16 [4096, 1024], replicated
- wv: bfloat16 [4096, 1024], replicated
- wo: bfloat16 [6144, 4096], replicated
Outputs:
- output: bfloat16 [4096, 4096], P(('dp', 'sp')), parts along dimension 0
There are 2 independent parts. The reference program is written for one: setup_inputs(seed, part) draws one part's arguments, and reference() takes and returns one part's arrays. A program takes and returns all parts, laid end to end along the dimension named above; an argument that names none is the same for every part.
All inputs are finite; a program needn't handle non-finite values.
Results may differ from the reference program's by a relative error of at most 0.012.
Values are sent between devices in bfloat16 or wider.
A program may use at most 768 MiB of HBM per device.

```python
import jax
import jax.numpy as jnp
from jax import lax

ROWS = 2048
D = 4096
HEADS = 48
KV_HEADS = 8
HEAD = 128
THETA = 10000


def setup_inputs(seed: int = 0, part: int = 0) -> dict:
    kx, kn, kq, kk, kv, ko = jax.random.split(jax.random.key(seed), 6)

    def weights(key, rows, columns):
        return jax.random.normal(key, (rows, columns), jnp.float32) * rows**-0.5

    drawn = {
        "x": jax.random.normal(jax.random.fold_in(kx, part), (ROWS, D), jnp.float32),
        "gain": 1 + 0.1 * jax.random.normal(kn, (D,), jnp.float32),
        "wq": 2 * weights(kq, D, HEADS * HEAD),
        "wk": 2 * weights(kk, D, KV_HEADS * HEAD),
        "wv": 4 * weights(kv, D, KV_HEADS * HEAD),
        "wo": weights(ko, HEADS * HEAD, D),
    }
    return {k: v.astype(jnp.bfloat16) for k, v in drawn.items()}


def normed(x, gain):
    wide = x.astype(jnp.float32)
    scale = lax.rsqrt(jnp.mean(wide * wide, -1, keepdims=True) + 1e-6)
    return (wide * scale * gain.astype(jnp.float32)).astype(jnp.bfloat16)


def turned(t, place, theta):
    half = t.shape[-1] // 2
    angle = place.astype(jnp.float32)[:, None] * theta ** (-jnp.arange(half, dtype=jnp.float32) / half)
    cos, sin = jnp.cos(angle)[:, None], jnp.sin(angle)[:, None]
    a, b = t[..., :half].astype(jnp.float32), t[..., half:].astype(jnp.float32)
    return jnp.concatenate([a * cos - b * sin, b * cos + a * sin], -1).astype(jnp.bfloat16)


def matmul(a, w):
    return jnp.dot(a, w, preferred_element_type=jnp.float32).astype(jnp.bfloat16)


def einsum(form, a, b):
    return jnp.einsum(form, a.astype(jnp.float32), b.astype(jnp.float32))


def attention(q, k, v):
    scores = einsum("tgsd,ugd->gstu", q, k) * q.shape[-1] ** -0.5
    token = jnp.arange(q.shape[0])
    scores = jnp.where(token[:, None] >= token, scores, -jnp.inf)
    weights = jax.nn.softmax(scores, -1).astype(jnp.bfloat16)
    return einsum("gstu,ugd->tgsd", weights, v).astype(jnp.bfloat16)


def reference(x, gain, wq, wk, wv, wo):
    a, place = normed(x, gain), jnp.arange(ROWS)
    q = turned(matmul(a, wq).reshape(ROWS, HEADS, HEAD), place, THETA).reshape(ROWS, KV_HEADS, -1, HEAD)
    k = turned(matmul(a, wk).reshape(ROWS, KV_HEADS, HEAD), place, THETA)
    v = matmul(a, wv).reshape(ROWS, KV_HEADS, HEAD)
    seen = attention(q, k, v).reshape(ROWS, HEADS * HEAD)
    return (x.astype(jnp.float32) + jnp.dot(seen, wo, preferred_element_type=jnp.float32)).astype(jnp.bfloat16)
```

```python
import functools

import jax
import jax.numpy as jnp
from jax import lax
from jax.experimental import pallas as pl
from jax.experimental.pallas import tpu as pltpu
from jax.sharding import PartitionSpec as P

HEAD = 128
THETA = 10000
HIDDEN = -2e30
LOG2E = 1.4426950408889634
DEPTH = 2048
WIDE = 512
SLOTS = 16
MESH = pl.DeviceIdType.MESH


def _dot(a, b, ca=1, cb=0):
    return lax.dot_general(a, b, (((ca,), (cb,)), ((), ())), preferred_element_type=jnp.float32)


def _kernel(n, x_hbm, gain_ref, turn_ref, wq, wk, wv, wo, y_hbm, x_s, a_s, ring, kv_s, q_s, acc_s, top_s, o_s, bias_s,
            x_sem, y_sem, ring_sem, send_sem, recv_sem):
    own, d = x_s.shape
    heads, kv_heads = q_s.shape[0], kv_s.shape[1]
    group, half = heads // kv_heads, kv_heads // 2
    per = WIDE // HEAD
    e = HEAD**-0.5 * LOG2E
    me = lax.axis_index("sp")
    chips = n // 2
    core, chip = lax.rem(me, 2), lax.div(me, 2)
    right_chip, left_chip = lax.rem(chip + 1, chips), lax.rem(chip + chips - 1, chips)
    far_chip = lax.rem(chip + 2, chips)
    partner, right, left = chip * 2 + 1 - core, right_chip * 2 + core, left_chip * 2 + core

    rows = d // DEPTH
    o_rows = wo.shape[0] // DEPTH
    kv_chunks = kv_heads // per
    q_chunks, o_chunks = heads // per, wo.shape[1] // WIDE
    q_first = 2 * kv_chunks * rows
    o_first = q_first + q_chunks * rows

    def fetch(src, part, chunk, slot):
        slot = slot % SLOTS if isinstance(slot, int) else lax.rem(slot, SLOTS)
        return pltpu.make_async_copy(src.at[pl.ds(part * DEPTH, DEPTH), pl.ds(chunk * WIDE, WIDE)], ring.at[slot], ring_sem.at[slot])

    def fetch_static(slot):
        if slot < q_first:
            c, part = slot // rows, slot % rows
            return fetch((wk, wv)[c % 2], part, c // 2, slot)
        if slot < o_first:
            c, part = (slot - q_first) // rows, (slot - q_first) % rows
            return fetch(wq, part, c, slot)
        c, part = (slot - o_first) // o_rows, (slot - o_first) % o_rows
        return fetch(wo, part, c, slot)

    def fetch_wq(c, part):
        return fetch(wq, part, c, q_first + rows * c + part)

    def fetch_wo(t):
        return fetch(wo, lax.rem(t, o_rows), lax.div(t, o_rows), o_first + t)

    x_copy = pltpu.make_async_copy(x_hbm, x_s, x_sem)
    x_copy.start()
    for slot in range(SLOTS):
        fetch_static(slot).start()

    barrier = pltpu.get_barrier_semaphore()
    for peer in (partner, right, left):
        pl.semaphore_signal(barrier, inc=1, device_id={"sp": peer}, device_id_type=MESH)

    def push(owner, h, slot, to, lane):
        ref = kv_s.at[owner, pl.ds(h * half, half)]
        return pltpu.make_async_remote_copy(ref, ref, send_sem.at[slot, lane], recv_sem.at[slot, lane], device_id={"sp": to},
                                            device_id_type=MESH)

    left_block, right_block, far_block = left_chip * 2 + core, right_chip * 2 + core, far_chip * 2 + core
    left_mate, right_mate, far_mate = left_chip * 2 + 1 - core, right_chip * 2 + 1 - core, far_chip * 2 + 1 - core
    mate = partner

    x_copy.wait()

    def norm(i, _):
        at = pl.ds(i * 32, 32)
        wide = x_s[at, :].astype(jnp.float32)
        scale = lax.rsqrt(jnp.mean(wide * wide, -1, keepdims=True) + 1e-6)
        a_s[at, :] = (wide * scale * gain_ref[...].astype(jnp.float32)).astype(jnp.bfloat16)
        return _

    lax.fori_loop(0, own // 32, norm, None)

    def project(first):
        total = None
        for part in range(rows):
            slot = (first + part) % SLOTS if isinstance(first, int) else lax.rem(first + part, SLOTS)
            pltpu.make_async_copy(wq.at[pl.ds(0, DEPTH), pl.ds(0, WIDE)], ring.at[slot], ring_sem.at[slot]).wait()
        for part in range(rows):
            slot = (first + part) % SLOTS if isinstance(first, int) else lax.rem(first + part, SLOTS)
            term = _dot(a_s[:, part * DEPTH : (part + 1) * DEPTH], ring[slot])
            total = term if total is None else total + term
        return total.astype(jnp.bfloat16)

    def turned(t):
        t = t.astype(jnp.float32)
        return (t * turn_ref[0] + pltpu.roll(t, HEAD // 2, 1) * turn_ref[1]).astype(jnp.bfloat16)

    def keys(c):
        t = project(2 * c * rows)
        for i in range(per):
            kv_s[me, c * per + i, 0] = turned(t[:, i * HEAD : (i + 1) * HEAD])
        for part in range(rows):
            fetch_static(2 * c * rows + part + SLOTS).start()

    def values(c):
        t = project((2 * c + 1) * rows)
        for i in range(per):
            for b in range(own // HEAD):
                square = t[b * HEAD : (b + 1) * HEAD, i * HEAD : (i + 1) * HEAD]
                kv_s[me, c * per + i, 1, b * HEAD : (b + 1) * HEAD, :] = square.T
        for part in range(rows):
            fetch_static((2 * c + 1) * rows + part + SLOTS).start()

    def queries(c):
        t = project(q_first + c * rows)
        for i in range(per):
            q_s[c * per + i] = turned(t[:, i * HEAD : (i + 1) * HEAD])

    keys(0)
    values(0)
    keys(1)
    pl.semaphore_wait(barrier, 3)
    push(me, 0, 1, right, 0).start()
    push(me, 0, 0, partner, 0).start()
    values(1)

    ahead = SLOTS // rows
    queries(0)
    push(me, 1, 2, left, 1).start()
    push(me, 1, 1, right, 1).start()
    push(me, 0, 2, left, 0).start()
    push(me, 1, 0, partner, 1).start()
    for part in range(rows):
        fetch_wq(ahead, part).start()

    def early(c, _):
        queries(c)
        for part in range(rows):
            fetch_wq(c + ahead, part).start()
        return _

    def late(c, _):
        queries(c)
        for part in range(rows):
            fetch_wo(rows * (c + ahead - q_chunks) + part).start()
        return _

    lax.fori_loop(1, q_chunks - ahead, early, None)
    lax.fori_loop(q_chunks - ahead, q_chunks, late, None)

    span = 2 * own
    place = lax.broadcasted_iota(jnp.int32, (span, own), 1) - lax.broadcasted_iota(jnp.int32, (span, own), 0) + core * own
    bias_s[...] = jnp.where(place >= 0, 0.0, HIDDEN)
    ones = jnp.ones((8, span), jnp.bfloat16)

    def step(c, h, first):
        def head(g, _):
            k = jnp.concatenate([kv_s[2 * c, g, 0], kv_s[2 * c + 1, g, 0]], axis=0)
            squares = [kv_s[2 * c + i, g, 1, b * HEAD : (b + 1) * HEAD, :] for i in range(2) for b in range(own // HEAD)]
            v = jnp.concatenate([jnp.concatenate(squares, axis=1), ones], axis=0)
            scores = lambda i: _dot(k, q_s[g * group + i], 1, 1)
            s = scores(0)
            for i in range(group):
                later = scores(i + 1) if i + 1 < group else None
                at = g * group + i
                if first:
                    s = s + bias_s[...]
                    top = s.max(axis=0, keepdims=True)
                else:
                    old = top_s[at]
                    top = jnp.maximum(old, s.max(axis=0, keepdims=True))
                p = jnp.exp2((s - top) * e).astype(jnp.bfloat16)
                mix = _dot(v, p)
                acc_s[at] = mix if first else acc_s[at] * jnp.exp2((old - top) * e) + mix
                top_s[at] = top
                s = later
            return _

        lax.fori_loop(h * half, (h + 1) * half, head, None)

    def arrive(owner, h, slot, lane):
        push(owner, h, slot, me, lane).wait_recv()

    arrive(left_block, 0, 1, 0)
    push(left_block, 0, 3, right, 0).start()
    push(left_block, 0, 4, partner, 0).start()
    arrive(right_block, 1, 2, 1)
    push(right_block, 1, 3, left, 1).start()
    push(right_block, 1, 5, partner, 1).start()

    for h in range(2):
        arrive(mate, h, 0, h)
        step(chip, h, True)

    def other(c, h):
        @pl.when(c < chip)
        def _():
            step(c, h, False)

    arrive(left_mate, 0, 4, 0)
    other(left_chip, 0)
    arrive(right_mate, 1, 5, 1)
    other(right_chip, 1)

    arrive(left_block, 1, 1, 1)
    push(left_block, 1, 4, partner, 1).start()
    arrive(right_block, 0, 2, 0)
    push(right_block, 0, 5, partner, 0).start()
    arrive(left_mate, 1, 4, 1)
    other(left_chip, 1)
    arrive(right_mate, 0, 5, 0)
    other(right_chip, 0)

    for h in range(2):
        arrive(far_block, h, 3, h)
        push(far_block, h, 6, partner, h).start()
    for h in range(2):
        arrive(far_mate, h, 6, h)
        other(far_chip, h)

    def finish(g, _):
        for i in range(group):
            mix = acc_s[g * group + i]
            out = (mix[:HEAD] * (1 / mix[HEAD : HEAD + 1])).astype(jnp.bfloat16)
            o_s[:, pl.ds(pl.multiple_of((g * group + i) * HEAD, HEAD), HEAD)] = out.T
        return _

    lax.fori_loop(0, kv_heads, finish, None)

    def result(c):
        at = pl.ds(pl.multiple_of(c * WIDE, WIDE), WIDE)
        return pltpu.make_async_copy(x_s.at[:, at], y_hbm.at[:, at], y_sem.at[c])

    def out(c, _):
        at = pl.ds(pl.multiple_of(c * WIDE, WIDE), WIDE)
        total = x_s[:, at].astype(jnp.float32)
        for part in range(o_rows):
            fetch_wo(o_rows * c + part).wait()
        mixed = None
        for part in range(o_rows):
            term = _dot(o_s[:, part * DEPTH : (part + 1) * DEPTH], ring[lax.rem(o_first + o_rows * c + part, SLOTS)])
            mixed = term if mixed is None else mixed + term
        x_s[:, at] = (total + mixed).astype(jnp.bfloat16)
        for part in range(o_rows):
            t = o_rows * c + part + SLOTS

            @pl.when(t < o_rows * o_chunks)
            def _():
                fetch_wo(t).start()

        result(c).start()
        return _

    lax.fori_loop(0, o_chunks, out, None)
    for c in range(o_chunks):
        result(c).wait()

    for h in range(2):
        for slot in (0, 1, 2, 4, 5, 6):
            push(me, h, slot, partner, h).wait_send()
        push(me, h, 3, partner, h).wait_send()


def solution(mesh):
    n = mesh.shape["sp"]

    def step(x, gain, wq, wk, wv, wo):
        own, d = x.shape
        heads, kv_heads = wq.shape[1] // HEAD, wk.shape[1] // HEAD
        half = HEAD // 2
        place = lax.axis_index("sp") * own + jnp.arange(own)
        angle = place.astype(jnp.float32)[:, None] * THETA ** (-jnp.arange(half, dtype=jnp.float32) / half)
        cos, sin = jnp.cos(angle), jnp.sin(angle)
        turn = jnp.stack([jnp.concatenate([cos, cos], -1), jnp.concatenate([-sin, sin], -1)])
        anywhere = pl.BlockSpec(memory_space=pl.ANY)
        vmem = pl.BlockSpec(memory_space=pltpu.VMEM)
        bf16, f32 = jnp.bfloat16, jnp.float32
        return pl.pallas_call(
            functools.partial(_kernel, n),
            out_shape=jax.ShapeDtypeStruct((own, d), bf16),
            in_specs=[anywhere, vmem, vmem, anywhere, anywhere, anywhere, anywhere],
            out_specs=anywhere,
            scratch_shapes=[
                pltpu.VMEM((own, d), bf16),
                pltpu.VMEM((own, d), bf16),
                pltpu.VMEM((SLOTS, DEPTH, WIDE), bf16),
                pltpu.VMEM((n, kv_heads, 2, own, HEAD), bf16),
                pltpu.VMEM((heads, own, HEAD), bf16),
                pltpu.VMEM((heads, HEAD + 8, own), f32),
                pltpu.VMEM((heads, 1, own), f32),
                pltpu.VMEM((own, heads * HEAD), bf16),
                pltpu.VMEM((2 * own, own), f32),
                pltpu.SemaphoreType.DMA,
                pltpu.SemaphoreType.DMA((wo.shape[1] // WIDE,)),
                pltpu.SemaphoreType.DMA((SLOTS,)),
                pltpu.SemaphoreType.DMA((7, 2)),
                pltpu.SemaphoreType.DMA((7, 2)),
            ],
            compiler_params=pltpu.CompilerParams(collective_id=0, has_side_effects=True, vmem_limit_bytes=67043328),
            cost_estimate=pl.CostEstimate(flops=2 * own * d * (2 * wq.shape[1] + 2 * wk.shape[1]), transcendentals=heads * own * own * n,
                                          bytes_accessed=2 * (2 * wq.size + 2 * wk.size)),
        )(x, gain.reshape(1, d), turn, wq, wk, wv, wo)

    tokens, whole = P(("dp", "sp"), None), P(None, None)
    return jax.shard_map(
        step,
        mesh=mesh,
        in_specs=(tokens, P(None), whole, whole, whole, whole),
        out_specs=tokens,
        check_vma=False,
    )
```

```python
import functools

import jax
import jax.numpy as jnp
from jax import lax
from jax.experimental import pallas as pl
from jax.experimental.pallas import tpu as pltpu
from jax.sharding import PartitionSpec as P

HEAD = 128
THETA = 10000
HIDDEN = -2e30
LOG2E = 1.4426950408889634
DEPTH = 2048
WIDE = 512
SLOTS = 12
MESH = pl.DeviceIdType.MESH


def _dot(a, b, ca=1, cb=0):
    return lax.dot_general(a, b, (((ca,), (cb,)), ((), ())), preferred_element_type=jnp.float32)


def _kernel(n, x_hbm, gain_ref, cos_ref, sin_ref, wq, wk, wv, wo, y_hbm, x_s, a_s, ring, kv_s, q_s, acc_s, top_s, o_s, bias_s,
            raw_s, sum_s, s0_s, s1_s, p0_s, p1_s, t0_s, t1_s, r0_s, r1_s, x_sem, y_sem, ring_sem, send_sem, recv_sem):
    own, d = x_s.shape
    heads, kv_heads = q_s.shape[0], kv_s.shape[1]
    group, half = heads // kv_heads, kv_heads // 2
    per = WIDE // HEAD
    e = HEAD**-0.5 * LOG2E
    me = lax.axis_index("sp")
    chips = n // 2
    core, chip = lax.rem(me, 2), lax.div(me, 2)
    right_chip, left_chip = lax.rem(chip + 1, chips), lax.rem(chip + chips - 1, chips)
    far_chip = lax.rem(chip + 2, chips)
    partner, right, left = chip * 2 + 1 - core, right_chip * 2 + core, left_chip * 2 + core

    rows = d // DEPTH
    o_rows = wo.shape[0] // DEPTH
    kv_chunks = kv_heads // per
    q_chunks, o_chunks = heads // per, wo.shape[1] // WIDE
    q_first = 2 * kv_chunks * rows
    o_first = q_first + q_chunks * rows
    ahead = SLOTS // rows
    reload = o_chunks - SLOTS // o_rows

    def fetch(src, part, chunk, slot):
        slot = slot % SLOTS if isinstance(slot, int) else lax.rem(slot, SLOTS)
        return pltpu.make_async_copy(src.at[pl.ds(part * DEPTH, DEPTH), pl.ds(chunk * WIDE, WIDE)], ring.at[slot], ring_sem.at[slot])

    def fetch_static(slot):
        if slot < q_first:
            c, part = slot // rows, slot % rows
            return fetch((wk, wv)[c % 2], part, c // 2, slot)
        c, part = (slot - q_first) // rows, (slot - q_first) % rows
        return fetch(wq, part, c, slot)

    def fetch_wq(c, part):
        return fetch(wq, part, c, q_first + rows * c + part)

    def fetch_wo(t):
        return fetch(wo, lax.rem(t, o_rows), lax.div(t, o_rows), o_first + t)

    def fetch_range(first, last):
        for slot in range(first, last):
            fetch_static(slot).start()

    x_copy = pltpu.make_async_copy(x_hbm, x_s, x_sem)
    x_copy.start()
    fetch_range(0, rows)

    barrier = pltpu.get_barrier_semaphore()
    for peer in (partner, right, left):
        pl.semaphore_signal(barrier, inc=1, device_id={"sp": peer}, device_id_type=MESH)

    def push(owner, h, slot, to, lane):
        ref = kv_s.at[owner, pl.ds(h * half, half)]
        return pltpu.make_async_remote_copy(ref, ref, send_sem.at[slot, lane], recv_sem.at[slot, lane], device_id={"sp": to},
                                            device_id_type=MESH)

    left_block, right_block, far_block = left_chip * 2 + core, right_chip * 2 + core, far_chip * 2 + core
    left_mate, right_mate, far_mate = left_chip * 2 + 1 - core, right_chip * 2 + 1 - core, far_chip * 2 + 1 - core

    x_copy.wait()
    fetch_range(rows, 4 * rows)

    def norm(i, _):
        at = pl.ds(i * 32, 32)
        wide = x_s[at, :].astype(jnp.float32)
        scale = lax.rsqrt(jnp.mean(wide * wide, -1, keepdims=True) + 1e-6)
        a_s[at, :] = (wide * scale * gain_ref[:1, :]).astype(jnp.bfloat16)
        return _

    lax.fori_loop(0, own // 32, norm, None)
    fetch_range(4 * rows, SLOTS)

    def slot_of(first, part):
        return (first + part) % SLOTS if isinstance(first, int) else lax.rem(first + part, SLOTS)

    def project(first, before):
        for part in range(rows):
            slot = slot_of(first, part)
            pltpu.make_async_copy(wq.at[pl.ds(0, DEPTH), pl.ds(0, WIDE)], ring.at[slot], ring_sem.at[slot]).wait()
        before()
        total = None
        for part in range(rows):
            term = _dot(a_s[:, part * DEPTH : (part + 1) * DEPTH], ring[slot_of(first, part)])
            total = term if total is None else total + term
        raw_s[...] = total.astype(jnp.bfloat16)

    def turned(i):
        t = raw_s[:, i * HEAD : (i + 1) * HEAD].astype(jnp.float32)
        return (t * cos_ref[...] + pltpu.roll(t, HEAD // 2, 1) * sin_ref[...]).astype(jnp.bfloat16)

    def keys(c):
        for i in range(per):
            kv_s[me, c * per + i, 0] = turned(i)

    def values(c):
        for i in range(per):
            for b in range(own // HEAD):
                kv_s[me, c * per + i, 1, b * HEAD : (b + 1) * HEAD, :] = raw_s[b * HEAD : (b + 1) * HEAD, i * HEAD : (i + 1) * HEAD].T

    def queries(c):
        for i in range(per):
            q_s[c * per + i] = turned(i)

    project(0, lambda: None)
    fetch_range(SLOTS, SLOTS + rows)
    project(rows, lambda: keys(0))
    fetch_range(SLOTS + rows, SLOTS + 2 * rows)
    project(2 * rows, lambda: values(0))
    fetch_range(SLOTS + 2 * rows, SLOTS + 3 * rows)
    pl.semaphore_wait(barrier, 3)
    push(me, 0, 1, right, 0).start()
    push(me, 0, 0, partner, 0).start()
    project(3 * rows, lambda: keys(1))
    fetch_range(SLOTS + 3 * rows, SLOTS + 4 * rows)
    project(q_first, lambda: values(1))
    push(me, 1, 2, left, 1).start()
    push(me, 1, 1, right, 1).start()
    push(me, 0, 2, left, 0).start()
    push(me, 1, 0, partner, 1).start()
    for part in range(rows):
        fetch_wq(ahead, part).start()

    def early(c, _):
        project(q_first + rows * c, lambda: queries(c - 1))
        for part in range(rows):
            fetch_wq(c + ahead, part).start()
        return _

    def late(c, _):
        project(q_first + rows * c, lambda: queries(c - 1))
        for part in range(rows):
            fetch_wo(rows * (c + ahead - q_chunks) + part).start()
        return _

    lax.fori_loop(1, q_chunks - ahead, early, None)
    lax.fori_loop(q_chunks - ahead, q_chunks, late, None)
    queries(q_chunks - 1)

    span = 2 * own
    place = lax.broadcasted_iota(jnp.int32, (span, own), 1) - lax.broadcasted_iota(jnp.int32, (span, own), 0) + core * own
    bias_s[...] = jnp.where(place >= 0, 0.0, HIDDEN)
    pairs = group // 2
    units = half * pairs
    s_s, p_s, t_s, r_s = (s0_s, s1_s), (p0_s, p1_s), (t0_s, t1_s), (r0_s, r1_s)

    def attend(where, count, first):
        def scores(u, slot):
            c, g, j = where(u)
            k = jnp.concatenate([kv_s[2 * c, g, 0], kv_s[2 * c + 1, g, 0]], axis=0)
            at = g * pairs + j
            s = _dot(k, q_s[pl.ds(2 * at, 2)].reshape(2 * own, HEAD), 1, 1)
            if first:
                s = s + jnp.concatenate([bias_s[...], bias_s[...]], axis=1)
            s_s[slot][...] = s
            top = s.max(axis=0, keepdims=True)
            if not first:
                old = top_s[at]
                top = jnp.maximum(old, top)
                r_s[slot][...] = jnp.exp2((old - top) * e)
            top_s[at] = top
            t_s[slot][...] = top

        def weights(slot):
            p_s[slot][...] = jnp.exp2((s_s[slot][...] - t_s[slot][...]) * e).astype(jnp.bfloat16)

        def mix(u, slot):
            c, g, j = where(u)
            squares = [kv_s[2 * c + i, g, 1, b * HEAD : (b + 1) * HEAD, :] for i in range(2) for b in range(own // HEAD)]
            v = jnp.concatenate([jnp.concatenate(squares, axis=1), jnp.ones((8, span), jnp.bfloat16)], axis=0)
            at = g * pairs + j
            new = _dot(v, p_s[slot][...])
            acc_s[at] = new if first else acc_s[at] * r_s[slot][...] + new

        def body(i, _):
            for k in range(2):
                mix(2 * i + k, k)
                scores(2 * i + k + 2, k)
                weights(1 - k)
            return _

        scores(0, 0)
        scores(1, 1)
        weights(0)
        lax.fori_loop(0, count // 2 - 1 if isinstance(count, int) else lax.div(count, 2) - 1, body, None)
        mix(count - 2, 0)
        weights(1)
        mix(count - 1, 1)

    def pieces(list_of):
        def where(u):
            c, h = list_of[0]
            if len(list_of) > 1:
                c, h = (jnp.where(u < units, one, two) for one, two in zip(*list_of))
                u = lax.rem(u, units)
            return c, h * half + lax.div(u, pairs), lax.rem(u, pairs)

        return where

    def arrive(owner, h, slot, lane):
        push(owner, h, slot, me, lane).wait_recv()

    arrive(left_block, 0, 1, 0)
    push(left_block, 0, 3, right, 0).start()
    push(left_block, 0, 4, partner, 0).start()
    arrive(right_block, 1, 2, 1)
    push(right_block, 1, 3, left, 1).start()
    push(right_block, 1, 5, partner, 1).start()

    for h in range(2):
        arrive(partner, h, 0, h)
    attend(pieces([(chip, 0), (chip, 1)]), 2 * units, True)

    def seen(c):
        return jnp.where(c < chip, units, 0)

    def both(one, two):
        count = seen(one[0]) + seen(two[0])

        @pl.when(count > 0)
        def _():
            attend(pieces([one, two]), count, False)

    arrive(left_mate, 0, 4, 0)
    arrive(right_mate, 1, 5, 1)
    both((left_chip, 0), (right_chip, 1))

    arrive(left_block, 1, 1, 1)
    push(left_block, 1, 4, partner, 1).start()
    arrive(right_block, 0, 2, 0)
    push(right_block, 0, 5, partner, 0).start()
    arrive(left_mate, 1, 4, 1)
    arrive(right_mate, 0, 5, 0)
    both((left_chip, 1), (right_chip, 0))

    for h in range(2):
        arrive(far_block, h, 3, h)
        push(far_block, h, 6, partner, h).start()
    for h in range(2):
        arrive(far_mate, h, 6, h)
    both((far_chip, 0), (far_chip, 1))

    def finish(at, _):
        for i in range(2):
            mixed = acc_s[at, :, i * own : (i + 1) * own]
            out = (mixed[:HEAD] * (1 / mixed[HEAD : HEAD + 1])).astype(jnp.bfloat16)
            o_s[:, pl.ds(pl.multiple_of((2 * at + i) * HEAD, HEAD), HEAD)] = out.T
        return _

    lax.fori_loop(0, heads // 2, finish, None)

    def columns(c):
        return pl.ds(pl.multiple_of(c * WIDE, WIDE), WIDE)

    def result(c):
        return pltpu.make_async_copy(x_s.at[:, columns(c)], y_hbm.at[:, columns(c)], y_sem.at[c])

    def add(c):
        x_s[:, columns(c)] = (x_s[:, columns(c)].astype(jnp.float32) + sum_s[...]).astype(jnp.bfloat16)

    def out(c, last, more):
        for part in range(o_rows):
            fetch_wo(o_rows * c + part).wait()
        if last is not None:
            add(last)
        total = None
        for part in range(o_rows):
            term = _dot(o_s[:, part * DEPTH : (part + 1) * DEPTH], ring[lax.rem(o_first + o_rows * c + part, SLOTS)])
            total = term if total is None else total + term
        sum_s[...] = total
        if more:
            for part in range(o_rows):
                fetch_wo(o_rows * c + part + SLOTS).start()
        if last is not None:
            result(last).start()

    def out_loop(more):
        def body(c, _):
            out(c, c - 1, more)
            return _

        return body

    out(0, None, True)
    lax.fori_loop(1, reload, out_loop(True), None)
    lax.fori_loop(reload, o_chunks, out_loop(False), None)
    add(o_chunks - 1)
    result(o_chunks - 1).start()
    for c in range(o_chunks):
        result(c).wait()

    for h in range(2):
        for slot in range(7):
            push(me, h, slot, partner, h).wait_send()


def solution(mesh):
    n = mesh.shape["sp"]

    def step(x, gain, wq, wk, wv, wo):
        own, d = x.shape
        heads, kv_heads = wq.shape[1] // HEAD, wk.shape[1] // HEAD
        half = HEAD // 2
        place = lax.axis_index("sp") * own + jnp.arange(own)
        lane = jnp.arange(HEAD)
        angle = place.astype(jnp.float32)[:, None] * THETA ** (-(lane % half).astype(jnp.float32) / half)
        cos, sin = jnp.cos(angle), jnp.where(lane < half, -1.0, 1.0) * jnp.sin(angle)
        wide_gain = jnp.broadcast_to(gain.astype(jnp.float32), (8, d))
        anywhere = pl.BlockSpec(memory_space=pl.ANY)
        vmem = pl.BlockSpec(memory_space=pltpu.VMEM)
        bf16, f32 = jnp.bfloat16, jnp.float32
        pairs, span = heads // 2, 2 * own
        return pl.pallas_call(
            functools.partial(_kernel, n),
            out_shape=jax.ShapeDtypeStruct((own, d), bf16),
            in_specs=[anywhere, vmem, vmem, vmem, anywhere, anywhere, anywhere, anywhere],
            out_specs=anywhere,
            scratch_shapes=[
                pltpu.VMEM((own, d), bf16),
                pltpu.VMEM((own, d), bf16),
                pltpu.VMEM((SLOTS, DEPTH, WIDE), bf16),
                pltpu.VMEM((n, kv_heads, 2, own, HEAD), bf16),
                pltpu.VMEM((heads, own, HEAD), bf16),
                pltpu.VMEM((pairs, HEAD + 8, span), f32),
                pltpu.VMEM((pairs, 1, span), f32),
                pltpu.VMEM((own, heads * HEAD), bf16),
                pltpu.VMEM((span, own), f32),
                pltpu.VMEM((own, WIDE), bf16),
                pltpu.VMEM((own, WIDE), f32),
                pltpu.VMEM((span, span), f32),
                pltpu.VMEM((span, span), f32),
                pltpu.VMEM((span, span), bf16),
                pltpu.VMEM((span, span), bf16),
                pltpu.VMEM((1, span), f32),
                pltpu.VMEM((1, span), f32),
                pltpu.VMEM((1, span), f32),
                pltpu.VMEM((1, span), f32),
                pltpu.SemaphoreType.DMA,
                pltpu.SemaphoreType.DMA((wo.shape[1] // WIDE,)),
                pltpu.SemaphoreType.DMA((SLOTS,)),
                pltpu.SemaphoreType.DMA((7, 2)),
                pltpu.SemaphoreType.DMA((7, 2)),
            ],
            compiler_params=pltpu.CompilerParams(collective_id=0, has_side_effects=True, vmem_limit_bytes=67043328),
            cost_estimate=pl.CostEstimate(flops=2 * own * d * (2 * wq.shape[1] + 2 * wk.shape[1]), transcendentals=heads * own * own * n,
                                          bytes_accessed=2 * (2 * wq.size + 2 * wk.size)),
        )(x, wide_gain, cos, sin, wq, wk, wv, wo)

    tokens, whole = P(("dp", "sp"), None), P(None, None)
    return jax.shard_map(
        step,
        mesh=mesh,
        in_specs=(tokens, P(None), whole, whole, whole, whole),
        out_specs=tokens,
        check_vma=False,
    )
```

```python
import functools

import jax
import jax.numpy as jnp
from jax import lax
from jax.experimental import pallas as pl
from jax.experimental.pallas import tpu as pltpu
from jax.sharding import PartitionSpec as P

HEAD = 128
THETA = 10000
HIDDEN = -2e30
LOG2E = 1.4426950408889634
DEPTH = 2048
WIDE = 512
SLOTS = 12
MESH = pl.DeviceIdType.MESH


def _dot(a, b, ca=1, cb=0):
    return lax.dot_general(a, b, (((ca,), (cb,)), ((), ())), preferred_element_type=jnp.float32)


def _kernel(n, x_hbm, gain_ref, cos_ref, sin_ref, wq, wk, wv, wo, y_hbm, x_s, a_s, ring, kv_s, q_s, acc_s, top_s, o_s, bias_s,
            raw_s, sum_s, s0_s, s1_s, p0_s, p1_s, t0_s, t1_s, r0_s, r1_s, x_sem, y_sem, ring_sem, send_sem, recv_sem):
    own, d = x_s.shape
    heads, kv_heads = q_s.shape[0], kv_s.shape[1]
    group, half = heads // kv_heads, kv_heads // 2
    per = WIDE // HEAD
    e = HEAD**-0.5 * LOG2E
    me = lax.axis_index("sp")
    chips = n // 2
    core, chip = lax.rem(me, 2), lax.div(me, 2)
    right_chip, left_chip = lax.rem(chip + 1, chips), lax.rem(chip + chips - 1, chips)
    far_chip = lax.rem(chip + 2, chips)
    partner, right, left = chip * 2 + 1 - core, right_chip * 2 + core, left_chip * 2 + core

    rows = d // DEPTH
    o_rows = wo.shape[0] // DEPTH
    kv_chunks = kv_heads // per
    q_chunks, o_chunks = heads // per, wo.shape[1] // WIDE
    q_first = 2 * kv_chunks * rows
    o_first = q_first + q_chunks * rows
    ahead = SLOTS // rows
    reload = o_chunks - SLOTS // o_rows

    def fetch(src, part, chunk, slot):
        slot = slot % SLOTS if isinstance(slot, int) else lax.rem(slot, SLOTS)
        return pltpu.make_async_copy(src.at[pl.ds(part * DEPTH, DEPTH), pl.ds(chunk * WIDE, WIDE)], ring.at[slot], ring_sem.at[slot])

    def fetch_static(slot):
        if slot < q_first:
            c, part = slot // rows, slot % rows
            return fetch((wk, wv)[c % 2], part, c // 2, slot)
        c, part = (slot - q_first) // rows, (slot - q_first) % rows
        return fetch(wq, part, c, slot)

    def fetch_wq(c, part):
        return fetch(wq, part, c, q_first + rows * c + part)

    def fetch_wo(t):
        return fetch(wo, lax.rem(t, o_rows), lax.div(t, o_rows), o_first + t)

    def fetch_range(first, last):
        for slot in range(first, last):
            fetch_static(slot).start()

    x_copy = pltpu.make_async_copy(x_hbm, x_s, x_sem)
    x_copy.start()
    fetch_range(0, rows)

    barrier = pltpu.get_barrier_semaphore()
    for peer in (partner, right, left):
        pl.semaphore_signal(barrier, inc=1, device_id={"sp": peer}, device_id_type=MESH)

    def push(owner, h, slot, to, lane):
        ref = kv_s.at[owner, pl.ds(h * half, half)]
        return pltpu.make_async_remote_copy(ref, ref, send_sem.at[slot, lane], recv_sem.at[slot, lane], device_id={"sp": to},
                                            device_id_type=MESH)

    left_block, right_block, far_block = left_chip * 2 + core, right_chip * 2 + core, far_chip * 2 + core
    left_mate, right_mate, far_mate = left_chip * 2 + 1 - core, right_chip * 2 + 1 - core, far_chip * 2 + 1 - core

    x_copy.wait()
    fetch_range(rows, 4 * rows)

    def norm(i, _):
        at = pl.ds(i * 32, 32)
        wide = x_s[at, :].astype(jnp.float32)
        scale = lax.rsqrt(jnp.mean(wide * wide, -1, keepdims=True) + 1e-6)
        a_s[at, :] = (wide * scale * gain_ref[:1, :]).astype(jnp.bfloat16)
        return _

    lax.fori_loop(0, own // 32, norm, None)
    fetch_range(4 * rows, SLOTS)

    def slot_of(first, part):
        return (first + part) % SLOTS if isinstance(first, int) else lax.rem(first + part, SLOTS)

    def project(first, before):
        for part in range(rows):
            slot = slot_of(first, part)
            pltpu.make_async_copy(wq.at[pl.ds(0, DEPTH), pl.ds(0, WIDE)], ring.at[slot], ring_sem.at[slot]).wait()
        before()
        total = None
        for part in range(rows):
            term = _dot(a_s[:, part * DEPTH : (part + 1) * DEPTH], ring[slot_of(first, part)])
            total = term if total is None else total + term
        raw_s[...] = total.astype(jnp.bfloat16)

    def turned(i):
        t = raw_s[:, i * HEAD : (i + 1) * HEAD].astype(jnp.float32)
        return (t * cos_ref[...] + pltpu.roll(t, HEAD // 2, 1) * sin_ref[...]).astype(jnp.bfloat16)

    def keys(c):
        for i in range(per):
            kv_s[me, c * per + i, 0] = turned(i)

    def values(c):
        for i in range(per):
            for b in range(own // HEAD):
                kv_s[me, c * per + i, 1, b * HEAD : (b + 1) * HEAD, :] = raw_s[b * HEAD : (b + 1) * HEAD, i * HEAD : (i + 1) * HEAD].T

    def queries(c):
        for i in range(per):
            q_s[c * per + i] = turned(i)

    def kv(c, _):
        project(2 * rows * c, lambda: values(jnp.maximum(c - 1, 0)))
        for part in range(rows):
            fetch_wq(2 * c + ahead - 2 * kv_chunks, part).start()

        @pl.when(c == kv_chunks - 1)
        def _():
            pl.semaphore_wait(barrier, 3)
            push(me, 0, 1, right, 0).start()
            push(me, 0, 0, partner, 0).start()

        project(2 * rows * c + rows, lambda: keys(c))
        for part in range(rows):
            fetch_wq(2 * c + 1 + ahead - 2 * kv_chunks, part).start()
        return _

    lax.fori_loop(0, kv_chunks, kv, None)
    values(kv_chunks - 1)

    def query(c, _):
        project(q_first + rows * c, lambda: queries(jnp.maximum(c - 1, 0)))

        @pl.when(c == 0)
        def _():
            push(me, 1, 2, left, 1).start()
            push(me, 1, 1, right, 1).start()
            push(me, 0, 2, left, 0).start()
            push(me, 1, 0, partner, 1).start()

        @pl.when(c < q_chunks - ahead)
        def _():
            for part in range(rows):
                fetch_wq(c + ahead, part).start()

        @pl.when(c >= q_chunks - ahead)
        def _():
            for part in range(rows):
                fetch_wo(rows * (c + ahead - q_chunks) + part).start()

        return _

    lax.fori_loop(0, q_chunks, query, None)
    queries(q_chunks - 1)

    span = 2 * own
    place = lax.broadcasted_iota(jnp.int32, (span, own), 1) - lax.broadcasted_iota(jnp.int32, (span, own), 0) + core * own
    bias_s[...] = jnp.where(place >= 0, 0.0, HIDDEN)
    pairs = group // 2
    units = half * pairs
    s_s, p_s, t_s, r_s = (s0_s, s1_s), (p0_s, p1_s), (t0_s, t1_s), (r0_s, r1_s)

    def attend(where, count, first):
        def scores(u, slot):
            c, g, j = where(u)
            k = jnp.concatenate([kv_s[2 * c, g, 0], kv_s[2 * c + 1, g, 0]], axis=0)
            at = g * pairs + j
            s = _dot(k, q_s[pl.ds(2 * at, 2)].reshape(2 * own, HEAD), 1, 1)
            if first:
                s = s + jnp.concatenate([bias_s[...], bias_s[...]], axis=1)
            s_s[slot][...] = s
            top = s.max(axis=0, keepdims=True)
            if not first:
                old = top_s[at]
                top = jnp.maximum(old, top)
                r_s[slot][...] = jnp.exp2((old - top) * e)
            top_s[at] = top
            t_s[slot][...] = top

        def weights(slot):
            p_s[slot][...] = jnp.exp2((s_s[slot][...] - t_s[slot][...]) * e).astype(jnp.bfloat16)

        def mix(u, slot):
            c, g, j = where(u)
            squares = [kv_s[2 * c + i, g, 1, b * HEAD : (b + 1) * HEAD, :] for i in range(2) for b in range(own // HEAD)]
            v = jnp.concatenate([jnp.concatenate(squares, axis=1), jnp.ones((8, span), jnp.bfloat16)], axis=0)
            at = g * pairs + j
            new = _dot(v, p_s[slot][...])
            acc_s[at] = new if first else acc_s[at] * r_s[slot][...] + new

        def body(i, _):
            for k in range(2):
                mix(2 * i + k, k)
                scores(2 * i + k + 2, k)
                weights(1 - k)
            return _

        scores(0, 0)
        scores(1, 1)
        weights(0)
        lax.fori_loop(0, count // 2 - 1 if isinstance(count, int) else lax.div(count, 2) - 1, body, None)
        mix(count - 2, 0)
        weights(1)
        mix(count - 1, 1)

    def pieces(list_of):
        def where(u):
            c, h = list_of[0]
            if len(list_of) > 1:
                c, h = (jnp.where(u < units, one, two) for one, two in zip(*list_of))
                u = lax.rem(u, units)
            return c, h * half + lax.div(u, pairs), lax.rem(u, pairs)

        return where

    def arrive(owner, h, slot, lane):
        push(owner, h, slot, me, lane).wait_recv()

    arrive(left_block, 0, 1, 0)
    push(left_block, 0, 3, right, 0).start()
    push(left_block, 0, 4, partner, 0).start()
    arrive(right_block, 1, 2, 1)
    push(right_block, 1, 3, left, 1).start()
    push(right_block, 1, 5, partner, 1).start()

    for h in range(2):
        arrive(partner, h, 0, h)
    attend(pieces([(chip, 0), (chip, 1)]), chip * 0 + 2 * units, True)

    def seen(c):
        return jnp.where(c < chip, units, 0)

    def others(turn, _):
        @pl.when(turn == 0)
        def _():
            arrive(left_mate, 0, 4, 0)
            arrive(right_mate, 1, 5, 1)

        @pl.when(turn == 1)
        def _():
            arrive(left_block, 1, 1, 1)
            push(left_block, 1, 4, partner, 1).start()
            arrive(right_block, 0, 2, 0)
            push(right_block, 0, 5, partner, 0).start()
            arrive(left_mate, 1, 4, 1)
            arrive(right_mate, 0, 5, 0)

        @pl.when(turn == 2)
        def _():
            for h in range(2):
                arrive(far_block, h, 3, h)
                push(far_block, h, 6, partner, h).start()
            for h in range(2):
                arrive(far_mate, h, 6, h)

        one, two = jnp.where(turn == 2, far_chip, left_chip), jnp.where(turn == 2, far_chip, right_chip)
        h = lax.rem(turn, 2)
        count = seen(one) + seen(two)

        @pl.when(count > 0)
        def _():
            attend(pieces([(one, h), (two, 1 - h)]), count, False)

        return _

    lax.fori_loop(0, 3, others, None)

    def finish(at, _):
        for i in range(2):
            mixed = acc_s[at, :, i * own : (i + 1) * own]
            out = (mixed[:HEAD] * (1 / mixed[HEAD : HEAD + 1])).astype(jnp.bfloat16)
            o_s[:, pl.ds(pl.multiple_of((2 * at + i) * HEAD, HEAD), HEAD)] = out.T
        return _

    lax.fori_loop(0, heads // 2, finish, None)

    def columns(c):
        return pl.ds(pl.multiple_of(c * WIDE, WIDE), WIDE)

    def result(c):
        return pltpu.make_async_copy(x_s.at[:, columns(c)], y_hbm.at[:, columns(c)], y_sem.at[c])

    def add(c):
        x_s[:, columns(c)] = (x_s[:, columns(c)].astype(jnp.float32) + sum_s[...]).astype(jnp.bfloat16)

    def out(c, _):
        for part in range(o_rows):
            fetch_wo(o_rows * c + part).wait()
        last = jnp.maximum(c - 1, 0)
        add(last)
        total = None
        for part in range(o_rows):
            term = _dot(o_s[:, part * DEPTH : (part + 1) * DEPTH], ring[lax.rem(o_first + o_rows * c + part, SLOTS)])
            total = term if total is None else total + term
        sum_s[...] = total

        @pl.when(c < reload)
        def _():
            for part in range(o_rows):
                fetch_wo(o_rows * c + part + SLOTS).start()

        @pl.when(c > 0)
        def _():
            result(last).start()

        return _

    sum_s[...] = jnp.zeros_like(sum_s)
    lax.fori_loop(0, o_chunks, out, None)
    add(o_chunks - 1)
    result(o_chunks - 1).start()
    for c in range(o_chunks):
        result(c).wait()

    for h in range(2):
        for slot in range(7):
            push(me, h, slot, partner, h).wait_send()


def solution(mesh):
    n = mesh.shape["sp"]

    def step(x, gain, wq, wk, wv, wo):
        own, d = x.shape
        heads, kv_heads = wq.shape[1] // HEAD, wk.shape[1] // HEAD
        half = HEAD // 2
        place = lax.axis_index("sp") * own + jnp.arange(own)
        lane = jnp.arange(HEAD)
        angle = place.astype(jnp.float32)[:, None] * THETA ** (-(lane % half).astype(jnp.float32) / half)
        cos, sin = jnp.cos(angle), jnp.where(lane < half, -1.0, 1.0) * jnp.sin(angle)
        wide_gain = jnp.broadcast_to(gain.astype(jnp.float32), (8, d))
        anywhere = pl.BlockSpec(memory_space=pl.ANY)
        vmem = pl.BlockSpec(memory_space=pltpu.VMEM)
        bf16, f32 = jnp.bfloat16, jnp.float32
        pairs, span = heads // 2, 2 * own
        return pl.pallas_call(
            functools.partial(_kernel, n),
            out_shape=jax.ShapeDtypeStruct((own, d), bf16),
            in_specs=[anywhere, vmem, vmem, vmem, anywhere, anywhere, anywhere, anywhere],
            out_specs=anywhere,
            scratch_shapes=[
                pltpu.VMEM((own, d), bf16),
                pltpu.VMEM((own, d), bf16),
                pltpu.VMEM((SLOTS, DEPTH, WIDE), bf16),
                pltpu.VMEM((n, kv_heads, 2, own, HEAD), bf16),
                pltpu.VMEM((heads, own, HEAD), bf16),
                pltpu.VMEM((pairs, HEAD + 8, span), f32),
                pltpu.VMEM((pairs, 1, span), f32),
                pltpu.VMEM((own, heads * HEAD), bf16),
                pltpu.VMEM((span, own), f32),
                pltpu.VMEM((own, WIDE), bf16),
                pltpu.VMEM((own, WIDE), f32),
                pltpu.VMEM((span, span), f32),
                pltpu.VMEM((span, span), f32),
                pltpu.VMEM((span, span), bf16),
                pltpu.VMEM((span, span), bf16),
                pltpu.VMEM((1, span), f32),
                pltpu.VMEM((1, span), f32),
                pltpu.VMEM((1, span), f32),
                pltpu.VMEM((1, span), f32),
                pltpu.SemaphoreType.DMA,
                pltpu.SemaphoreType.DMA((wo.shape[1] // WIDE,)),
                pltpu.SemaphoreType.DMA((SLOTS,)),
                pltpu.SemaphoreType.DMA((7, 2)),
                pltpu.SemaphoreType.DMA((7, 2)),
            ],
            compiler_params=pltpu.CompilerParams(collective_id=0, has_side_effects=True, vmem_limit_bytes=67043328),
            cost_estimate=pl.CostEstimate(flops=2 * own * d * (2 * wq.shape[1] + 2 * wk.shape[1]), transcendentals=heads * own * own * n,
                                          bytes_accessed=2 * (2 * wq.size + 2 * wk.size)),
        )(x, wide_gain, cos, sin, wq, wk, wv, wo)

    tokens, whole = P(("dp", "sp"), None), P(None, None)
    return jax.shard_map(
        step,
        mesh=mesh,
        in_specs=(tokens, P(None), whole, whole, whole, whole),
        out_specs=tokens,
        check_vma=False,
    )
```

```python
import functools

import jax
import jax.numpy as jnp
from jax import lax
from jax.experimental import pallas as pl
from jax.experimental.pallas import tpu as pltpu
from jax.sharding import PartitionSpec as P

HEAD = 128
THETA = 10000
HIDDEN = -2e30
LOG2E = 1.4426950408889634
DEPTH = 2048
WIDE = 512
SLOTS = 12
MESH = pl.DeviceIdType.MESH


def _dot(a, b, ca=1, cb=0):
    return lax.dot_general(a, b, (((ca,), (cb,)), ((), ())), preferred_element_type=jnp.float32)


def _kernel(n, x_hbm, gain_hbm, rate_hbm, wq, wk, wv, wo, y_hbm, x_s, a_s, ring, kv_s, q_s, acc_s, top_s, o_s, bias_s,
            raw_s, sum_s, s0_s, s1_s, p0_s, p1_s, t0_s, t1_s, r0_s, r1_s, gain_s, rate_s, cos_s, sin_s, x_sem, small_sem, y_sem, ring_sem, send_sem, recv_sem):
    own, d = x_s.shape
    heads, kv_heads = q_s.shape[0], kv_s.shape[2]
    group, half = heads // kv_heads, kv_heads // 2
    per = WIDE // HEAD
    e = HEAD**-0.5 * LOG2E
    me = lax.axis_index("sp")
    chips = n // 2
    core, chip = lax.rem(me, 2), lax.div(me, 2)
    right_chip, left_chip = lax.rem(chip + 1, chips), lax.rem(chip + chips - 1, chips)
    far_chip = lax.rem(chip + 2, chips)
    partner, right, left = chip * 2 + 1 - core, right_chip * 2 + core, left_chip * 2 + core

    rows = d // DEPTH
    o_rows = wo.shape[0] // DEPTH
    kv_chunks = kv_heads // per
    q_chunks, o_chunks = heads // per, wo.shape[1] // WIDE
    q_first = 2 * kv_chunks * rows
    o_first = q_first + q_chunks * rows
    ahead = SLOTS // rows
    reload = o_chunks - SLOTS // o_rows

    def fetch(src, part, chunk, slot):
        slot = slot % SLOTS if isinstance(slot, int) else lax.rem(slot, SLOTS)
        return pltpu.make_async_copy(src.at[pl.ds(part * DEPTH, DEPTH), pl.ds(chunk * WIDE, WIDE)], ring.at[slot], ring_sem.at[slot])

    def fetch_static(slot):
        if slot < q_first:
            c, part = slot // rows, slot % rows
            return fetch((wk, wv)[c % 2], part, c // 2, slot)
        c, part = (slot - q_first) // rows, (slot - q_first) % rows
        return fetch(wq, part, c, slot)

    def fetch_wq(c, part):
        return fetch(wq, part, c, q_first + rows * c + part)

    def fetch_wo(t):
        return fetch(wo, lax.rem(t, o_rows), lax.div(t, o_rows), o_first + t)

    def fetch_range(first, last):
        for slot in range(first, last):
            fetch_static(slot).start()

    x_copy = pltpu.make_async_copy(x_hbm, x_s, x_sem)
    x_copy.start()
    small = [pltpu.make_async_copy(gain_hbm, gain_s, small_sem.at[0]), pltpu.make_async_copy(rate_hbm, rate_s, small_sem.at[1])]
    for copy in small:
        copy.start()
    fetch_range(0, rows)

    barrier = pltpu.get_barrier_semaphore()
    for peer in (partner, right, left):
        pl.semaphore_signal(barrier, inc=1, device_id={"sp": peer}, device_id_type=MESH)

    def push_part(owner, h, slot, to, lane, part):
        ref = kv_s.at[owner, part, pl.ds(h * half, half)]
        return pltpu.make_async_remote_copy(ref, ref, send_sem.at[slot, lane, part], recv_sem.at[slot, lane, part], device_id={"sp": to},
                                            device_id_type=MESH)

    def push(owner, h, slot, to, lane):
        for part in range(2):
            push_part(owner, h, slot, to, lane, part).start()

    left_block, right_block, far_block = left_chip * 2 + core, right_chip * 2 + core, far_chip * 2 + core
    left_mate, right_mate, far_mate = left_chip * 2 + 1 - core, right_chip * 2 + 1 - core, far_chip * 2 + 1 - core

    for copy in small:
        copy.wait()
    angle = (me * own + lax.broadcasted_iota(jnp.int32, (own, HEAD), 0)).astype(jnp.float32) * rate_s[:1, :]
    cos_s[...] = jnp.cos(angle)
    sin_s[...] = jnp.where(lax.broadcasted_iota(jnp.int32, (own, HEAD), 1) < HEAD // 2, -1.0, 1.0) * jnp.sin(angle)
    gain = jnp.concatenate([gain_s[i : i + 1, :].astype(jnp.float32) for i in range(d // HEAD)], axis=1)

    x_copy.wait()
    fetch_range(rows, 4 * rows)

    def norm(i, _):
        at = pl.ds(i * 32, 32)
        wide = x_s[at, :].astype(jnp.float32)
        scale = lax.rsqrt(jnp.mean(wide * wide, -1, keepdims=True) + 1e-6)
        a_s[at, :] = (wide * scale * gain).astype(jnp.bfloat16)
        return _

    lax.fori_loop(0, own // 32, norm, None)
    fetch_range(4 * rows, SLOTS)

    def slot_of(first, part):
        return (first + part) % SLOTS if isinstance(first, int) else lax.rem(first + part, SLOTS)

    def project(first, before):
        for part in range(rows):
            slot = slot_of(first, part)
            pltpu.make_async_copy(wq.at[pl.ds(0, DEPTH), pl.ds(0, WIDE)], ring.at[slot], ring_sem.at[slot]).wait()
        before()
        total = None
        for part in range(rows):
            term = _dot(a_s[:, part * DEPTH : (part + 1) * DEPTH], ring[slot_of(first, part)])
            total = term if total is None else total + term
        raw_s[...] = total.astype(jnp.bfloat16)

    def turned(i):
        t = raw_s[:, i * HEAD : (i + 1) * HEAD].astype(jnp.float32)
        return (t * cos_s[...] + pltpu.roll(t, HEAD // 2, 1) * sin_s[...]).astype(jnp.bfloat16)

    def keys(c):
        for i in range(per):
            kv_s[me, 0, c * per + i] = turned(i)

    def values(c):
        for i in range(per):
            for b in range(own // HEAD):
                kv_s[me, 1, c * per + i, b * HEAD : (b + 1) * HEAD, :] = raw_s[b * HEAD : (b + 1) * HEAD, i * HEAD : (i + 1) * HEAD].T

    def queries(c):
        for i in range(per):
            q_s[c * per + i] = turned(i)

    def kv(c, _):
        project(2 * rows * c, lambda: values(jnp.maximum(c - 1, 0)))
        for part in range(rows):
            fetch_wq(2 * c + ahead - 2 * kv_chunks, part).start()

        @pl.when(c == kv_chunks - 1)
        def _():
            push_part(me, 0, 1, right, 0, 1).start()
            push(me, 0, 0, partner, 0)

        project(2 * rows * c + rows, lambda: keys(c))

        @pl.when(c == 0)
        def _():
            push_part(me, 0, 1, right, 0, 0).start()

        for part in range(rows):
            fetch_wq(2 * c + 1 + ahead - 2 * kv_chunks, part).start()
        return _

    pl.semaphore_wait(barrier, 3)
    lax.fori_loop(0, kv_chunks, kv, None)
    push_part(me, 1, 2, left, 1, 0).start()
    values(kv_chunks - 1)

    def query(c, _):
        project(q_first + rows * c, lambda: queries(jnp.maximum(c - 1, 0)))

        @pl.when(c == 0)
        def _():
            push_part(me, 1, 2, left, 1, 1).start()
            push(me, 1, 1, right, 1)
            push(me, 0, 2, left, 0)
            push(me, 1, 0, partner, 1)

        @pl.when(c < q_chunks - ahead)
        def _():
            for part in range(rows):
                fetch_wq(c + ahead, part).start()

        @pl.when(c >= q_chunks - ahead)
        def _():
            for part in range(rows):
                fetch_wo(rows * (c + ahead - q_chunks) + part).start()

        return _

    lax.fori_loop(0, q_chunks, query, None)
    queries(q_chunks - 1)

    span = 2 * own
    place = lax.broadcasted_iota(jnp.int32, (span, own), 1) - lax.broadcasted_iota(jnp.int32, (span, own), 0) + core * own
    bias_s[...] = jnp.where(place >= 0, 0.0, HIDDEN)
    pairs = group // 2
    units = half * pairs
    s_s, p_s, t_s, r_s = (s0_s, s1_s), (p0_s, p1_s), (t0_s, t1_s), (r0_s, r1_s)

    def attend(where, count, first, before=None):
        def scores(u, slot):
            c, g, j = where(u)
            k = jnp.concatenate([kv_s[2 * c, 0, g], kv_s[2 * c + 1, 0, g]], axis=0)
            at = g * pairs + j
            s = _dot(k, q_s[pl.ds(2 * at, 2)].reshape(2 * own, HEAD), 1, 1)
            if first:
                s = s + jnp.concatenate([bias_s[...], bias_s[...]], axis=1)
            s_s[slot][...] = s
            top = s.max(axis=0, keepdims=True)
            if not first:
                old = top_s[at]
                top = jnp.maximum(old, top)
                r_s[slot][...] = jnp.exp2((old - top) * e)
            top_s[at] = top
            t_s[slot][...] = top

        def weights(slot):
            for r in range(0, span, span // 8):
                at = slice(r, r + span // 8)
                p_s[slot][at, :] = jnp.exp2((s_s[slot][at, :] - t_s[slot][...]) * e).astype(jnp.bfloat16)

        def mix(u, slot):
            c, g, j = where(u)
            squares = [kv_s[2 * c + i, 1, g, b * HEAD : (b + 1) * HEAD, :] for i in range(2) for b in range(own // HEAD)]
            v = jnp.concatenate([jnp.concatenate(squares, axis=1), jnp.ones((8, span), jnp.bfloat16)], axis=0)
            at = g * pairs + j
            new = _dot(v, p_s[slot][...])
            acc_s[at] = new if first else acc_s[at] * r_s[slot][...] + new

        def body(i, _):
            if before is not None:
                before(i)
            for k in range(2):
                mix(2 * i + k, k)
                scores(2 * i + k + 2, k)
                weights(1 - k)
            return _

        scores(0, 0)
        scores(1, 1)
        weights(0)
        lax.fori_loop(0, lax.div(count, 2) - 1, body, None)
        mix(count - 2, 0)
        weights(1)
        mix(count - 1, 1)

    def arrive(owner, h, slot, lane):
        for part in range(2):
            push_part(owner, h, slot, me, lane, part).wait_recv()

    arrive(left_block, 0, 1, 0)
    push(left_block, 0, 3, right, 0)
    push(left_block, 0, 4, partner, 0)
    arrive(right_block, 1, 2, 1)
    push(right_block, 1, 3, left, 1)
    push(right_block, 1, 5, partner, 1)

    for h in range(2):
        arrive(partner, h, 0, h)
    attend(lambda u: (chip, lax.div(u, pairs), lax.rem(u, pairs)), chip * 0 + 2 * units, True)

    def seen(c):
        return jnp.where(c < chip, units, 0)

    begin1 = seen(left_chip) + seen(right_chip)
    begin2 = 2 * begin1
    count = begin2 + 2 * seen(far_chip)

    def round0():
        arrive(left_mate, 0, 4, 0)
        arrive(right_mate, 1, 5, 1)

    def round1():
        arrive(left_block, 1, 1, 1)
        push(left_block, 1, 4, partner, 1)
        arrive(right_block, 0, 2, 0)
        push(right_block, 0, 5, partner, 0)
        arrive(left_mate, 1, 4, 1)
        arrive(right_mate, 0, 5, 0)

    def round2():
        for h in range(2):
            arrive(far_block, h, 3, h)
            push(far_block, h, 6, partner, h)
        for h in range(2):
            arrive(far_mate, h, 6, h)

    def where(u):
        turn = jnp.where(u < begin1, 0, jnp.where(u < begin2, 1, 2))
        u = u - jnp.where(turn == 0, 0, jnp.where(turn == 1, begin1, begin2))
        second = lax.div(u, units)
        c = jnp.where(turn == 2, far_chip, jnp.where(second == 0, left_chip, right_chip))
        h = lax.rem(turn + second, 2)
        u = u - second * units
        return c, h * half + lax.div(u, pairs), lax.rem(u, pairs)

    def before(i):
        @pl.when(lax.div(begin1, 2) - 1 == i)
        def _():
            round1()

        @pl.when((lax.div(begin2, 2) - 1 == i) & (begin2 < count))
        def _():
            round2()

    round0()

    @pl.when(count > 0)
    def _():
        attend(where, count, False, before)

    @pl.when(count == 0)
    def _():
        round1()

    @pl.when(begin2 == count)
    def _():
        round2()

    def finish(at, _):
        for i in range(2):
            mixed = acc_s[at, :, i * own : (i + 1) * own]
            out = (mixed[:HEAD] * (1 / mixed[HEAD : HEAD + 1])).astype(jnp.bfloat16)
            o_s[:, pl.ds(pl.multiple_of((2 * at + i) * HEAD, HEAD), HEAD)] = out.T
        return _

    lax.fori_loop(0, heads // 2, finish, None)

    def columns(c):
        return pl.ds(pl.multiple_of(c * WIDE, WIDE), WIDE)

    def result(c):
        return pltpu.make_async_copy(x_s.at[:, columns(c)], y_hbm.at[:, columns(c)], y_sem.at[c])

    def add(c):
        x_s[:, columns(c)] = (x_s[:, columns(c)].astype(jnp.float32) + sum_s[...]).astype(jnp.bfloat16)

    def out(c, _):
        for part in range(o_rows):
            fetch_wo(o_rows * c + part).wait()
        last = jnp.maximum(c - 1, 0)
        add(last)
        total = None
        for part in range(o_rows):
            term = _dot(o_s[:, part * DEPTH : (part + 1) * DEPTH], ring[lax.rem(o_first + o_rows * c + part, SLOTS)])
            total = term if total is None else total + term
        sum_s[...] = total

        @pl.when(c < reload)
        def _():
            for part in range(o_rows):
                fetch_wo(o_rows * c + part + SLOTS).start()

        @pl.when(c > 0)
        def _():
            result(last).start()

        return _

    sum_s[...] = jnp.zeros_like(sum_s)
    lax.fori_loop(0, o_chunks, out, None)
    add(o_chunks - 1)
    result(o_chunks - 1).start()
    for c in range(o_chunks):
        result(c).wait()

    for h in range(2):
        for slot in range(7):
            for part in range(2):
                push_part(me, h, slot, partner, h, part).wait_send()


def solution(mesh):
    n = mesh.shape["sp"]

    def step(x, gain, wq, wk, wv, wo):
        own, d = x.shape
        heads, kv_heads = wq.shape[1] // HEAD, wk.shape[1] // HEAD
        half = HEAD // 2
        rate = THETA ** (-(jnp.arange(HEAD) % half).astype(jnp.float32) / half)
        anywhere = pl.BlockSpec(memory_space=pl.ANY)
        bf16, f32 = jnp.bfloat16, jnp.float32
        pairs, span = heads // 2, 2 * own
        return pl.pallas_call(
            functools.partial(_kernel, n),
            out_shape=jax.ShapeDtypeStruct((own, d), bf16),
            in_specs=[anywhere] * 7,
            out_specs=anywhere,
            scratch_shapes=[
                pltpu.VMEM((own, d), bf16),
                pltpu.VMEM((own, d), bf16),
                pltpu.VMEM((SLOTS, DEPTH, WIDE), bf16),
                pltpu.VMEM((n, 2, kv_heads, own, HEAD), bf16),
                pltpu.VMEM((heads, own, HEAD), bf16),
                pltpu.VMEM((pairs, HEAD + 8, span), f32),
                pltpu.VMEM((pairs, 1, span), f32),
                pltpu.VMEM((own, heads * HEAD), bf16),
                pltpu.VMEM((span, own), f32),
                pltpu.VMEM((own, WIDE), bf16),
                pltpu.VMEM((own, WIDE), f32),
                pltpu.VMEM((span, span), f32),
                pltpu.VMEM((span, span), f32),
                pltpu.VMEM((span, span), bf16),
                pltpu.VMEM((span, span), bf16),
                pltpu.VMEM((1, span), f32),
                pltpu.VMEM((1, span), f32),
                pltpu.VMEM((1, span), f32),
                pltpu.VMEM((1, span), f32),
                pltpu.VMEM((d // HEAD, HEAD), bf16),
                pltpu.VMEM((8, HEAD), f32),
                pltpu.VMEM((own, HEAD), f32),
                pltpu.VMEM((own, HEAD), f32),
                pltpu.SemaphoreType.DMA,
                pltpu.SemaphoreType.DMA((2,)),
                pltpu.SemaphoreType.DMA((wo.shape[1] // WIDE,)),
                pltpu.SemaphoreType.DMA((SLOTS,)),
                pltpu.SemaphoreType.DMA((7, 2, 2)),
                pltpu.SemaphoreType.DMA((7, 2, 2)),
            ],
            compiler_params=pltpu.CompilerParams(collective_id=0, has_side_effects=True, vmem_limit_bytes=67043328),
            cost_estimate=pl.CostEstimate(flops=2 * own * d * (2 * wq.shape[1] + 2 * wk.shape[1]), transcendentals=heads * own * own * n,
                                          bytes_accessed=2 * (2 * wq.size + 2 * wk.size)),
        )(x, gain.reshape(d // HEAD, HEAD), jnp.broadcast_to(rate, (8, HEAD)), wq, wk, wv, wo)

    tokens, whole = P(("dp", "sp"), None), P(None, None)
    return jax.shard_map(
        step,
        mesh=mesh,
        in_specs=(tokens, P(None), whole, whole, whole, whole),
        out_specs=tokens,
        check_vma=False,
    )
```

```python
import functools

import jax
import jax.numpy as jnp
from jax import lax
from jax.experimental import pallas as pl
from jax.experimental.pallas import tpu as pltpu
from jax.sharding import PartitionSpec as P

HEAD = 128
THETA = 10000
HIDDEN = -2e30
LOG2E = 1.4426950408889634
DEPTH = 2048
WIDE = 512
SLOTS = 12
MESH = pl.DeviceIdType.MESH


def _dot(a, b, ca=1, cb=0):
    return lax.dot_general(a, b, (((ca,), (cb,)), ((), ())), preferred_element_type=jnp.float32)


def _kernel(n, x_hbm, gain_hbm, rate_hbm, wq, wk, wv, wo, y_hbm, x_s, a_s, ring, kv_s, q_s, acc_s, top_s, o_s, bias_s,
            raw_s, sum_s, s0_s, s1_s, p0_s, p1_s, t0_s, t1_s, r0_s, r1_s, gain_s, rate_s, cos_s, sin_s, x_sem, small_sem, y_sem, ring_sem, send_sem, recv_sem):
    own, d = x_s.shape
    heads, kv_heads = q_s.shape[0], kv_s.shape[2]
    group, half = heads // kv_heads, kv_heads // 2
    per = WIDE // HEAD
    e = HEAD**-0.5 * LOG2E
    me = lax.axis_index("sp")
    chips = n // 2
    core, chip = lax.rem(me, 2), lax.div(me, 2)
    right_chip, left_chip = lax.rem(chip + 1, chips), lax.rem(chip + chips - 1, chips)
    far_chip = lax.rem(chip + 2, chips)
    partner, right, left = chip * 2 + 1 - core, right_chip * 2 + core, left_chip * 2 + core

    rows = d // DEPTH
    o_rows = wo.shape[0] // DEPTH
    kv_chunks = kv_heads // per
    q_chunks, o_chunks = heads // per, wo.shape[1] // WIDE
    q_first = 2 * kv_chunks * rows
    o_first = q_first + q_chunks * rows
    ahead = SLOTS // rows
    reload = o_chunks - SLOTS // o_rows

    def fetch(src, part, chunk, slot):
        slot = slot % SLOTS if isinstance(slot, int) else lax.rem(slot, SLOTS)
        return pltpu.make_async_copy(src.at[pl.ds(part * DEPTH, DEPTH), pl.ds(chunk * WIDE, WIDE)], ring.at[slot], ring_sem.at[slot])

    def fetch_static(slot):
        if slot < q_first:
            c, part = slot // rows, slot % rows
            return fetch((wk, wv)[c % 2], part, c // 2, slot)
        c, part = (slot - q_first) // rows, (slot - q_first) % rows
        return fetch(wq, part, c, slot)

    def fetch_wq(c, part):
        return fetch(wq, part, c, q_first + rows * c + part)

    def fetch_wo(t):
        return fetch(wo, lax.rem(t, o_rows), lax.div(t, o_rows), o_first + t)

    def fetch_range(first, last):
        for slot in range(first, last):
            fetch_static(slot).start()

    x_copy = pltpu.make_async_copy(x_hbm, x_s, x_sem)
    x_copy.start()
    small = [pltpu.make_async_copy(gain_hbm, gain_s, small_sem.at[0]), pltpu.make_async_copy(rate_hbm, rate_s, small_sem.at[1])]
    for copy in small:
        copy.start()
    fetch_range(0, rows)

    barrier = pltpu.get_barrier_semaphore()
    for peer in (partner, right, left):
        pl.semaphore_signal(barrier, inc=1, device_id={"sp": peer}, device_id_type=MESH)

    def push_part(owner, h, slot, to, lane, part):
        ref = kv_s.at[owner, part, pl.ds(h * half, half)]
        return pltpu.make_async_remote_copy(ref, ref, send_sem.at[slot, lane, part], recv_sem.at[slot, lane, part], device_id={"sp": to},
                                            device_id_type=MESH)

    def push(owner, h, slot, to, lane):
        for part in range(2):
            push_part(owner, h, slot, to, lane, part).start()

    left_block, right_block, far_block = left_chip * 2 + core, right_chip * 2 + core, far_chip * 2 + core
    left_mate, right_mate, far_mate = left_chip * 2 + 1 - core, right_chip * 2 + 1 - core, far_chip * 2 + 1 - core

    for copy in small:
        copy.wait()
    angle = (me * own + lax.broadcasted_iota(jnp.int32, (own, HEAD), 0)).astype(jnp.float32) * rate_s[...]
    cos_s[...] = jnp.cos(angle)
    sin_s[...] = jnp.where(lax.broadcasted_iota(jnp.int32, (own, HEAD), 1) < HEAD // 2, -1.0, 1.0) * jnp.sin(angle)
    gain = jnp.concatenate([gain_s[i : i + 1, :].astype(jnp.float32) for i in range(d // HEAD)], axis=1)

    x_copy.wait()
    fetch_range(rows, 4 * rows)

    def norm(i, _):
        at = pl.ds(i * 32, 32)
        wide = x_s[at, :].astype(jnp.float32)
        scale = lax.rsqrt(jnp.mean(wide * wide, -1, keepdims=True) + 1e-6)
        a_s[at, :] = (wide * scale * gain).astype(jnp.bfloat16)
        return _

    lax.fori_loop(0, own // 32, norm, None)
    fetch_range(4 * rows, SLOTS)

    def slot_of(first, part):
        return (first + part) % SLOTS if isinstance(first, int) else lax.rem(first + part, SLOTS)

    def project(first, before):
        for part in range(rows):
            slot = slot_of(first, part)
            pltpu.make_async_copy(wq.at[pl.ds(0, DEPTH), pl.ds(0, WIDE)], ring.at[slot], ring_sem.at[slot]).wait()
        before()
        total = None
        for part in range(rows):
            term = _dot(a_s[:, part * DEPTH : (part + 1) * DEPTH], ring[slot_of(first, part)])
            total = term if total is None else total + term
        raw_s[...] = total.astype(jnp.bfloat16)

    def turned(i):
        t = raw_s[:, i * HEAD : (i + 1) * HEAD].astype(jnp.float32)
        return (t * cos_s[...] + pltpu.roll(t, HEAD // 2, 1) * sin_s[...]).astype(jnp.bfloat16)

    def keys(c):
        for i in range(per):
            kv_s[me, 0, c * per + i] = turned(i)

    def values(c):
        for i in range(per):
            for b in range(own // HEAD):
                kv_s[me, 1, c * per + i, b * HEAD : (b + 1) * HEAD, :] = raw_s[b * HEAD : (b + 1) * HEAD, i * HEAD : (i + 1) * HEAD].T

    def queries(c):
        for i in range(per):
            q_s[c * per + i] = turned(i)

    def kv(c, _):
        project(2 * rows * c, lambda: values(jnp.maximum(c - 1, 0)))
        for part in range(rows):
            fetch_wq(2 * c + ahead - 2 * kv_chunks, part).start()

        @pl.when(c == kv_chunks - 1)
        def _():
            push_part(me, 0, 1, right, 0, 1).start()
            push(me, 0, 0, partner, 0)

        project(2 * rows * c + rows, lambda: keys(c))

        @pl.when(c == 0)
        def _():
            push_part(me, 0, 1, right, 0, 0).start()

        for part in range(rows):
            fetch_wq(2 * c + 1 + ahead - 2 * kv_chunks, part).start()
        return _

    pl.semaphore_wait(barrier, 3)
    lax.fori_loop(0, kv_chunks, kv, None)
    push_part(me, 1, 2, left, 1, 0).start()
    values(kv_chunks - 1)

    def query(c, _):
        project(q_first + rows * c, lambda: queries(jnp.maximum(c - 1, 0)))

        @pl.when(c == 0)
        def _():
            push_part(me, 1, 2, left, 1, 1).start()
            push(me, 1, 1, right, 1)
            push(me, 0, 2, left, 0)
            push(me, 1, 0, partner, 1)

        @pl.when(c < q_chunks - ahead)
        def _():
            for part in range(rows):
                fetch_wq(c + ahead, part).start()

        @pl.when(c >= q_chunks - ahead)
        def _():
            for part in range(rows):
                fetch_wo(rows * (c + ahead - q_chunks) + part).start()

        return _

    lax.fori_loop(0, q_chunks, query, None)
    queries(q_chunks - 1)

    span = 2 * own
    place = lax.broadcasted_iota(jnp.int32, (span, own), 1) - lax.broadcasted_iota(jnp.int32, (span, own), 0) + core * own
    bias_s[...] = jnp.where(place >= 0, 0.0, HIDDEN)
    pairs = group // 2
    units = half * pairs
    s_s, p_s, t_s, r_s = (s0_s, s1_s), (p0_s, p1_s), (t0_s, t1_s), (r0_s, r1_s)

    def attend(where, count, first, before=None):
        def scores(unit, slot):
            c, g, at = unit
            k = jnp.concatenate([kv_s[2 * c, 0, g], kv_s[2 * c + 1, 0, g]], axis=0)
            s = _dot(k, q_s[pl.ds(2 * at, 2)].reshape(2 * own, HEAD), 1, 1)
            if first:
                s = s + jnp.concatenate([bias_s[...], bias_s[...]], axis=1)
            s_s[slot][...] = s
            top = s.max(axis=0, keepdims=True)
            if not first:
                old = top_s[at]
                top = jnp.maximum(old, top)
                r_s[slot][...] = jnp.exp2((old - top) * e)
            top_s[at] = top
            t_s[slot][...] = top

        def weights(slot):
            for r in range(0, span, span // 8):
                at = slice(r, r + span // 8)
                p_s[slot][at, :] = jnp.exp2((s_s[slot][at, :] - t_s[slot][...]) * e).astype(jnp.bfloat16)

        def mix(unit, slot):
            c, g, at = unit
            squares = [kv_s[2 * c + i, 1, g, b * HEAD : (b + 1) * HEAD, :] for i in range(2) for b in range(own // HEAD)]
            v = jnp.concatenate([jnp.concatenate(squares, axis=1), jnp.ones((8, span), jnp.bfloat16)], axis=0)
            new = _dot(v, p_s[slot][...])
            acc_s[at] = new if first else acc_s[at] * r_s[slot][...] + new

        def body(i, _):
            if before is not None:
                before(i)
            held = [where(2 * i + k) for k in range(4)]
            for k in range(2):
                mix(held[k], k)
                scores(held[k + 2], k)
                weights(1 - k)
            return _

        scores(where(0), 0)
        scores(where(1), 1)
        weights(0)
        lax.fori_loop(0, lax.div(count, 2) - 1, body, None)
        mix(where(count - 2), 0)
        weights(1)
        mix(where(count - 1), 1)

    def arrive(owner, h, slot, lane):
        for part in range(2):
            push_part(owner, h, slot, me, lane, part).wait_recv()

    arrive(left_block, 0, 1, 0)
    push(left_block, 0, 3, right, 0)
    push(left_block, 0, 4, partner, 0)
    arrive(right_block, 1, 2, 1)
    push(right_block, 1, 3, left, 1)
    push(right_block, 1, 5, partner, 1)

    for h in range(2):
        arrive(partner, h, 0, h)
    attend(lambda u: (chip, lax.div(jnp.int32(u), pairs), jnp.int32(u)), chip * 0 + 2 * units, True)

    def seen(c):
        return jnp.where(c < chip, units, 0)

    begin1 = seen(left_chip) + seen(right_chip)
    begin2 = 2 * begin1
    count = begin2 + 2 * seen(far_chip)

    def round0():
        arrive(left_mate, 0, 4, 0)
        arrive(right_mate, 1, 5, 1)

    def round1():
        arrive(left_block, 1, 1, 1)
        push(left_block, 1, 4, partner, 1)
        arrive(right_block, 0, 2, 0)
        push(right_block, 0, 5, partner, 0)
        arrive(left_mate, 1, 4, 1)
        arrive(right_mate, 0, 5, 0)

    def round2():
        for h in range(2):
            arrive(far_block, h, 3, h)
            push(far_block, h, 6, partner, h)
        for h in range(2):
            arrive(far_mate, h, 6, h)

    def where(u):
        turn = jnp.where(u < begin1, 0, jnp.where(u < begin2, 1, 2))
        u = u - jnp.where(turn == 0, 0, jnp.where(turn == 1, begin1, begin2))
        second = lax.div(u, units)
        c = jnp.where(turn == 2, far_chip, jnp.where(second == 0, left_chip, right_chip))
        h = lax.rem(turn + second, 2)
        u = u - second * units
        at = h * units + u
        return c, lax.div(at, pairs), at

    def before(i):
        @pl.when(lax.div(begin1, 2) - 1 == i)
        def _():
            round1()

        @pl.when((lax.div(begin2, 2) - 1 == i) & (begin2 < count))
        def _():
            round2()

    round0()

    @pl.when(count > 0)
    def _():
        attend(where, count, False, before)

    @pl.when(count == 0)
    def _():
        round1()

    @pl.when(begin2 == count)
    def _():
        round2()

    def finish(first, _):
        for i in range(8):
            at = first * 4 + i // 2
            mixed = acc_s[at, :, i % 2 * own : (i % 2 + 1) * own]
            out = (mixed[:HEAD] * (1 / mixed[HEAD : HEAD + 1])).astype(jnp.bfloat16)
            o_s[:, pl.ds(pl.multiple_of((first * 8 + i) * HEAD, HEAD), HEAD)] = out.T
        return _

    lax.fori_loop(0, heads // 8, finish, None)

    def columns(c):
        return pl.ds(pl.multiple_of(c * WIDE, WIDE), WIDE)

    def result(c):
        return pltpu.make_async_copy(x_s.at[:, columns(c)], y_hbm.at[:, columns(c)], y_sem.at[c])

    def add(c):
        x_s[:, columns(c)] = (x_s[:, columns(c)].astype(jnp.float32) + sum_s[...]).astype(jnp.bfloat16)

    def out(c, _):
        for part in range(o_rows):
            fetch_wo(o_rows * c + part).wait()
        last = jnp.maximum(c - 1, 0)
        add(last)
        total = None
        for part in range(o_rows):
            term = _dot(o_s[:, part * DEPTH : (part + 1) * DEPTH], ring[lax.rem(o_first + o_rows * c + part, SLOTS)])
            total = term if total is None else total + term
        sum_s[...] = total

        @pl.when(c < reload)
        def _():
            for part in range(o_rows):
                fetch_wo(o_rows * c + part + SLOTS).start()

        @pl.when(c > 0)
        def _():
            result(last).start()

        return _

    sum_s[...] = jnp.zeros_like(sum_s)
    lax.fori_loop(0, o_chunks, out, None)
    add(o_chunks - 1)
    result(o_chunks - 1).start()
    for c in range(o_chunks):
        result(c).wait()

    for h in range(2):
        for slot in range(7):
            for part in range(2):
                push_part(me, h, slot, partner, h, part).wait_send()


def solution(mesh):
    n = mesh.shape["sp"]

    def step(x, gain, wq, wk, wv, wo):
        own, d = x.shape
        heads, kv_heads = wq.shape[1] // HEAD, wk.shape[1] // HEAD
        half = HEAD // 2
        rate = THETA ** (-(jnp.arange(HEAD) % half).astype(jnp.float32) / half)
        anywhere = pl.BlockSpec(memory_space=pl.ANY)
        bf16, f32 = jnp.bfloat16, jnp.float32
        pairs, span = heads // 2, 2 * own
        return pl.pallas_call(
            functools.partial(_kernel, n),
            out_shape=jax.ShapeDtypeStruct((own, d), bf16),
            in_specs=[anywhere] * 7,
            out_specs=anywhere,
            scratch_shapes=[
                pltpu.VMEM((own, d), bf16),
                pltpu.VMEM((own, d), bf16),
                pltpu.VMEM((SLOTS, DEPTH, WIDE), bf16),
                pltpu.VMEM((n, 2, kv_heads, own, HEAD), bf16),
                pltpu.VMEM((heads, own, HEAD), bf16),
                pltpu.VMEM((pairs, HEAD + 8, span), f32),
                pltpu.VMEM((pairs, 1, span), f32),
                pltpu.VMEM((own, heads * HEAD), bf16),
                pltpu.VMEM((span, own), f32),
                pltpu.VMEM((own, WIDE), bf16),
                pltpu.VMEM((own, WIDE), f32),
                pltpu.VMEM((span, span), f32),
                pltpu.VMEM((span, span), f32),
                pltpu.VMEM((span, span), bf16),
                pltpu.VMEM((span, span), bf16),
                pltpu.VMEM((1, span), f32),
                pltpu.VMEM((1, span), f32),
                pltpu.VMEM((1, span), f32),
                pltpu.VMEM((1, span), f32),
                pltpu.VMEM((d // HEAD, HEAD), bf16),
                pltpu.VMEM((1, HEAD), f32),
                pltpu.VMEM((own, HEAD), f32),
                pltpu.VMEM((own, HEAD), f32),
                pltpu.SemaphoreType.DMA,
                pltpu.SemaphoreType.DMA((2,)),
                pltpu.SemaphoreType.DMA((wo.shape[1] // WIDE,)),
                pltpu.SemaphoreType.DMA((SLOTS,)),
                pltpu.SemaphoreType.DMA((7, 2, 2)),
                pltpu.SemaphoreType.DMA((7, 2, 2)),
            ],
            compiler_params=pltpu.CompilerParams(collective_id=0, has_side_effects=True, vmem_limit_bytes=67043328),
            cost_estimate=pl.CostEstimate(flops=2 * own * d * (2 * wq.shape[1] + 2 * wk.shape[1]), transcendentals=heads * own * own * n,
                                          bytes_accessed=2 * (2 * wq.size + 2 * wk.size)),
        )(x, gain.reshape(d // HEAD, HEAD), rate.reshape(1, HEAD), wq, wk, wv, wo)

    tokens, whole = P(("dp", "sp"), None), P(None, None)
    return jax.shard_map(
        step,
        mesh=mesh,
        in_specs=(tokens, P(None), whole, whole, whole, whole),
        out_specs=tokens,
        check_vma=False,
    )
```

```python
import functools

import jax
import jax.numpy as jnp
from jax import lax
from jax.experimental import pallas as pl
from jax.experimental.pallas import tpu as pltpu
from jax.sharding import PartitionSpec as P

HEAD = 128
THETA = 10000
HIDDEN = -2e30
LOG2E = 1.4426950408889634
DEPTH = 2048
WIDE = 512
SLOTS = 12
MESH = pl.DeviceIdType.MESH


def _dot(a, b, ca=1, cb=0):
    return lax.dot_general(a, b, (((ca,), (cb,)), ((), ())), preferred_element_type=jnp.float32)


def _kernel(n, x_hbm, gain_hbm, rate_hbm, wq, wk, wv, wo, y_hbm, x_s, a_s, ring, kv_s, q_s, acc_s, top_s, o_s, bias_s,
            raw_s, sum_s, s0_s, s1_s, p0_s, p1_s, t0_s, t1_s, r0_s, r1_s, gain_s, rate_s, cos_s, sin_s, x_sem, small_sem, y_sem, ring_sem, send_sem, recv_sem):
    own, d = x_s.shape
    heads, kv_heads = q_s.shape[0], kv_s.shape[2]
    group, half = heads // kv_heads, kv_heads // 2
    per = WIDE // HEAD
    e = HEAD**-0.5 * LOG2E
    me = lax.axis_index("sp")
    chips = n // 2
    core, chip = lax.rem(me, 2), lax.div(me, 2)
    right_chip, left_chip = lax.rem(chip + 1, chips), lax.rem(chip + chips - 1, chips)
    far_chip = lax.rem(chip + 2, chips)
    partner, right, left = chip * 2 + 1 - core, right_chip * 2 + core, left_chip * 2 + core

    rows = d // DEPTH
    o_rows = wo.shape[0] // DEPTH
    kv_chunks = kv_heads // per
    q_chunks, o_chunks = heads // per, wo.shape[1] // WIDE
    q_first = 2 * kv_chunks * rows
    o_first = q_first + q_chunks * rows
    ahead = SLOTS // rows
    reload = o_chunks - SLOTS // o_rows

    def fetch(src, part, chunk, slot):
        slot = slot % SLOTS if isinstance(slot, int) else lax.rem(slot, SLOTS)
        return pltpu.make_async_copy(src.at[pl.ds(part * DEPTH, DEPTH), pl.ds(chunk * WIDE, WIDE)], ring.at[slot], ring_sem.at[slot])

    def fetch_static(slot):
        if slot < q_first:
            c, part = slot // rows, slot % rows
            return fetch((wk, wv)[c % 2], part, c // 2, slot)
        c, part = (slot - q_first) // rows, (slot - q_first) % rows
        return fetch(wq, part, c, slot)

    def fetch_wq(c, part):
        return fetch(wq, part, c, q_first + rows * c + part)

    def fetch_wo(t):
        return fetch(wo, lax.rem(t, o_rows), lax.div(t, o_rows), o_first + t)

    def fetch_range(first, last):
        for slot in range(first, last):
            fetch_static(slot).start()

    x_copy = pltpu.make_async_copy(x_hbm, x_s, x_sem)
    x_copy.start()
    small = [pltpu.make_async_copy(gain_hbm, gain_s, small_sem.at[0]), pltpu.make_async_copy(rate_hbm, rate_s, small_sem.at[1])]
    for copy in small:
        copy.start()
    fetch_range(0, rows)

    barrier = pltpu.get_barrier_semaphore()
    for peer in (partner, right, left):
        pl.semaphore_signal(barrier, inc=1, device_id={"sp": peer}, device_id_type=MESH)

    def push_part(owner, h, slot, to, lane, part):
        ref = kv_s.at[owner, part, pl.ds(h * half, half)]
        return pltpu.make_async_remote_copy(ref, ref, send_sem.at[slot, lane, part], recv_sem.at[slot, lane, part], device_id={"sp": to},
                                            device_id_type=MESH)

    def push(owner, h, slot, to, lane):
        for part in range(2):
            push_part(owner, h, slot, to, lane, part).start()

    left_block, right_block, far_block = left_chip * 2 + core, right_chip * 2 + core, far_chip * 2 + core
    left_mate, right_mate, far_mate = left_chip * 2 + 1 - core, right_chip * 2 + 1 - core, far_chip * 2 + 1 - core

    for copy in small:
        copy.wait()
    angle = (me * own + lax.broadcasted_iota(jnp.int32, (own, HEAD), 0)).astype(jnp.float32) * rate_s[...]
    cos_s[...] = jnp.cos(angle)
    sin_s[...] = jnp.where(lax.broadcasted_iota(jnp.int32, (own, HEAD), 1) < HEAD // 2, -1.0, 1.0) * jnp.sin(angle)
    gain = jnp.concatenate([gain_s[i : i + 1, :].astype(jnp.float32) for i in range(d // HEAD)], axis=1)

    x_copy.wait()
    fetch_range(rows, 4 * rows)

    def norm(i, _):
        at = pl.ds(i * 32, 32)
        wide = x_s[at, :].astype(jnp.float32)
        scale = lax.rsqrt(jnp.mean(wide * wide, -1, keepdims=True) + 1e-6)
        a_s[at, :] = (wide * scale * gain).astype(jnp.bfloat16)
        return _

    lax.fori_loop(0, own // 32, norm, None)
    fetch_range(4 * rows, SLOTS)

    def slot_of(first, part):
        return (first + part) % SLOTS if isinstance(first, int) else lax.rem(first + part, SLOTS)

    def project(first, before):
        for part in range(rows):
            slot = slot_of(first, part)
            pltpu.make_async_copy(wq.at[pl.ds(0, DEPTH), pl.ds(0, WIDE)], ring.at[slot], ring_sem.at[slot]).wait()
        before()
        total = None
        for part in range(rows):
            term = _dot(a_s[:, part * DEPTH : (part + 1) * DEPTH], ring[slot_of(first, part)])
            total = term if total is None else total + term
        raw_s[...] = total.astype(jnp.bfloat16)

    def turned(i):
        t = raw_s[:, i * HEAD : (i + 1) * HEAD].astype(jnp.float32)
        return (t * cos_s[...] + pltpu.roll(t, HEAD // 2, 1) * sin_s[...]).astype(jnp.bfloat16)

    def keys(c):
        for i in range(per):
            kv_s[me, 0, c * per + i] = turned(i)

    def values(c):
        for i in range(per):
            for b in range(own // HEAD):
                kv_s[me, 1, c * per + i, b * HEAD : (b + 1) * HEAD, :] = raw_s[b * HEAD : (b + 1) * HEAD, i * HEAD : (i + 1) * HEAD].T

    def queries(c):
        for i in range(per):
            q_s[c * per + i] = turned(i)

    def kv(c, _):
        project(2 * rows * c, lambda: values(jnp.maximum(c - 1, 0)))
        for part in range(rows):
            fetch_wq(2 * c + ahead - 2 * kv_chunks, part).start()

        @pl.when(c == kv_chunks - 1)
        def _():
            push_part(me, 0, 1, right, 0, 1).start()
            push(me, 0, 0, partner, 0)

        project(2 * rows * c + rows, lambda: keys(c))

        @pl.when(c == 0)
        def _():
            push_part(me, 0, 1, right, 0, 0).start()

        for part in range(rows):
            fetch_wq(2 * c + 1 + ahead - 2 * kv_chunks, part).start()
        return _

    pl.semaphore_wait(barrier, 3)
    lax.fori_loop(0, kv_chunks, kv, None)
    push_part(me, 1, 2, left, 1, 0).start()
    values(kv_chunks - 1)

    def query(c, _):
        project(q_first + rows * c, lambda: queries(jnp.maximum(c - 1, 0)))

        @pl.when(c == 0)
        def _():
            push_part(me, 1, 2, left, 1, 1).start()
            push(me, 1, 1, right, 1)
            push(me, 0, 2, left, 0)
            push(me, 1, 0, partner, 1)

        @pl.when(c < q_chunks - ahead)
        def _():
            for part in range(rows):
                fetch_wq(c + ahead, part).start()

        @pl.when(c >= q_chunks - ahead)
        def _():
            for part in range(rows):
                fetch_wo(rows * (c + ahead - q_chunks) + part).start()

        return _

    lax.fori_loop(0, q_chunks, query, None)
    queries(q_chunks - 1)

    span = 2 * own
    place = lax.broadcasted_iota(jnp.int32, (span, own), 1) - lax.broadcasted_iota(jnp.int32, (span, own), 0) + core * own
    bias_s[...] = jnp.where(place >= 0, 0.0, HIDDEN)
    pairs = group // 2
    units = half * pairs
    s_s, p_s, t_s, r_s = (s0_s, s1_s), (p0_s, p1_s), (t0_s, t1_s), (r0_s, r1_s)

    def attend(where, count, first, before=None):
        def scores(unit, slot):
            c, g, at = unit
            k = jnp.concatenate([kv_s[2 * c, 0, g], kv_s[2 * c + 1, 0, g]], axis=0)
            s = _dot(k, q_s[pl.ds(2 * at, 2)].reshape(2 * own, HEAD), 1, 1)
            if first:
                s = s + jnp.concatenate([bias_s[...], bias_s[...]], axis=1)
            s_s[slot][...] = s
            top = s.max(axis=0, keepdims=True)
            if not first:
                old = top_s[at]
                top = jnp.maximum(old, top)
                r_s[slot][...] = jnp.exp2((old - top) * e)
            top_s[at] = top
            t_s[slot][...] = top

        def weights(slot):
            for r in range(0, span, span // 8):
                at = slice(r, r + span // 8)
                p_s[slot][at, :] = jnp.exp2((s_s[slot][at, :] - t_s[slot][...]) * e).astype(jnp.bfloat16)

        def mix(unit, slot):
            c, g, at = unit
            squares = [kv_s[2 * c + i, 1, g, b * HEAD : (b + 1) * HEAD, :] for i in range(2) for b in range(own // HEAD)]
            v = jnp.concatenate([jnp.concatenate(squares, axis=1), jnp.ones((8, span), jnp.bfloat16)], axis=0)
            new = _dot(v, p_s[slot][...])
            acc_s[at] = new if first else acc_s[at] * r_s[slot][...] + new

        def body(i, _):
            if before is not None:
                before(i)
            held = [where(6 * i + k) for k in range(6 + 2)]
            for k in range(6):
                mix(held[k], k % 2)
                scores(held[k + 2], k % 2)
                weights(1 - k % 2)
            return _

        scores(where(0), 0)
        scores(where(1), 1)
        weights(0)
        lax.fori_loop(0, lax.div(count, 6) - 1, body, None)
        for k in range(6, 2, -1):
            mix(where(count - k), k % 2)
            scores(where(count - k + 2), k % 2)
            weights(1 - k % 2)
        mix(where(count - 2), 0)
        weights(1)
        mix(where(count - 1), 1)

    def arrive(owner, h, slot, lane):
        for part in range(2):
            push_part(owner, h, slot, me, lane, part).wait_recv()

    arrive(left_block, 0, 1, 0)
    push(left_block, 0, 3, right, 0)
    push(left_block, 0, 4, partner, 0)
    arrive(right_block, 1, 2, 1)
    push(right_block, 1, 3, left, 1)
    push(right_block, 1, 5, partner, 1)

    for h in range(2):
        arrive(partner, h, 0, h)
    attend(lambda u: (chip, lax.div(jnp.int32(u), pairs), jnp.int32(u)), chip * 0 + 2 * units, True)

    def seen(c):
        return jnp.where(c < chip, units, 0)

    begin1 = seen(left_chip) + seen(right_chip)
    begin2 = 2 * begin1
    count = begin2 + 2 * seen(far_chip)

    def round0():
        arrive(left_mate, 0, 4, 0)
        arrive(right_mate, 1, 5, 1)

    def round1():
        arrive(left_block, 1, 1, 1)
        push(left_block, 1, 4, partner, 1)
        arrive(right_block, 0, 2, 0)
        push(right_block, 0, 5, partner, 0)
        arrive(left_mate, 1, 4, 1)
        arrive(right_mate, 0, 5, 0)

    def round2():
        for h in range(2):
            arrive(far_block, h, 3, h)
            push(far_block, h, 6, partner, h)
        for h in range(2):
            arrive(far_mate, h, 6, h)

    def where(u):
        turn = jnp.where(u < begin1, 0, jnp.where(u < begin2, 1, 2))
        u = u - jnp.where(turn == 0, 0, jnp.where(turn == 1, begin1, begin2))
        second = lax.div(u, units)
        c = jnp.where(turn == 2, far_chip, jnp.where(second == 0, left_chip, right_chip))
        h = lax.rem(turn + second, 2)
        u = u - second * units
        at = h * units + u
        return c, lax.div(at, pairs), at

    def before(i):
        @pl.when(lax.div(begin1 - 2, 6) == i)
        def _():
            round1()

        @pl.when((lax.div(begin2 - 2, 6) == i) & (begin2 < count))
        def _():
            round2()

    round0()

    @pl.when(count > 0)
    def _():
        attend(where, count, False, before)

    @pl.when(count == 0)
    def _():
        round1()

    @pl.when(begin2 == count)
    def _():
        round2()

    def finish(first, _):
        for i in range(8):
            at = first * 4 + i // 2
            mixed = acc_s[at, :, i % 2 * own : (i % 2 + 1) * own]
            out = (mixed[:HEAD] * (1 / mixed[HEAD : HEAD + 1])).astype(jnp.bfloat16)
            o_s[:, pl.ds(pl.multiple_of((first * 8 + i) * HEAD, HEAD), HEAD)] = out.T
        return _

    lax.fori_loop(0, heads // 8, finish, None)

    def columns(c):
        return pl.ds(pl.multiple_of(c * WIDE, WIDE), WIDE)

    def result(c):
        return pltpu.make_async_copy(x_s.at[:, columns(c)], y_hbm.at[:, columns(c)], y_sem.at[c])

    def add(c):
        x_s[:, columns(c)] = (x_s[:, columns(c)].astype(jnp.float32) + sum_s[...]).astype(jnp.bfloat16)

    def out(c, _):
        for part in range(o_rows):
            fetch_wo(o_rows * c + part).wait()
        last = jnp.maximum(c - 1, 0)
        add(last)
        total = None
        for part in range(o_rows):
            term = _dot(o_s[:, part * DEPTH : (part + 1) * DEPTH], ring[lax.rem(o_first + o_rows * c + part, SLOTS)])
            total = term if total is None else total + term
        sum_s[...] = total

        @pl.when(c < reload)
        def _():
            for part in range(o_rows):
                fetch_wo(o_rows * c + part + SLOTS).start()

        @pl.when(c > 0)
        def _():
            result(last).start()

        return _

    sum_s[...] = jnp.zeros_like(sum_s)
    lax.fori_loop(0, o_chunks, out, None)
    add(o_chunks - 1)
    result(o_chunks - 1).start()
    for c in range(o_chunks):
        result(c).wait()

    for h in range(2):
        for slot in range(7):
            for part in range(2):
                push_part(me, h, slot, partner, h, part).wait_send()


def _copy(a_ref, b_ref):
    b_ref[...] = a_ref[...]


def solution(mesh):
    n = mesh.shape["sp"]

    def step(x, gain, wq, wk, wv, wo):
        own, d = x.shape
        heads, kv_heads = wq.shape[1] // HEAD, wk.shape[1] // HEAD
        half = HEAD // 2
        rate = THETA ** (-(jnp.arange(HEAD) % half).astype(jnp.float32) / half)
        anywhere = pl.BlockSpec(memory_space=pl.ANY)
        bf16, f32 = jnp.bfloat16, jnp.float32
        pairs, span = heads // 2, 2 * own
        y = pl.pallas_call(
            functools.partial(_kernel, n),
            out_shape=jax.ShapeDtypeStruct((own, d), bf16),
            in_specs=[anywhere] * 7,
            out_specs=anywhere,
            scratch_shapes=[
                pltpu.VMEM((own, d), bf16),
                pltpu.VMEM((own, d), bf16),
                pltpu.VMEM((SLOTS, DEPTH, WIDE), bf16),
                pltpu.VMEM((n, 2, kv_heads, own, HEAD), bf16),
                pltpu.VMEM((heads, own, HEAD), bf16),
                pltpu.VMEM((pairs, HEAD + 8, span), f32),
                pltpu.VMEM((pairs, 1, span), f32),
                pltpu.VMEM((own, heads * HEAD), bf16),
                pltpu.VMEM((span, own), f32),
                pltpu.VMEM((own, WIDE), bf16),
                pltpu.VMEM((own, WIDE), f32),
                pltpu.VMEM((span, span), f32),
                pltpu.VMEM((span, span), f32),
                pltpu.VMEM((span, span), bf16),
                pltpu.VMEM((span, span), bf16),
                pltpu.VMEM((1, span), f32),
                pltpu.VMEM((1, span), f32),
                pltpu.VMEM((1, span), f32),
                pltpu.VMEM((1, span), f32),
                pltpu.VMEM((d // HEAD, HEAD), bf16),
                pltpu.VMEM((1, HEAD), f32),
                pltpu.VMEM((own, HEAD), f32),
                pltpu.VMEM((own, HEAD), f32),
                pltpu.SemaphoreType.DMA,
                pltpu.SemaphoreType.DMA((2,)),
                pltpu.SemaphoreType.DMA((wo.shape[1] // WIDE,)),
                pltpu.SemaphoreType.DMA((SLOTS,)),
                pltpu.SemaphoreType.DMA((7, 2, 2)),
                pltpu.SemaphoreType.DMA((7, 2, 2)),
            ],
            compiler_params=pltpu.CompilerParams(collective_id=0, has_side_effects=True, vmem_limit_bytes=67043328),
            cost_estimate=pl.CostEstimate(flops=2 * own * d * (2 * wq.shape[1] + 2 * wk.shape[1]), transcendentals=heads * own * own * n,
                                          bytes_accessed=2 * (2 * wq.size + 2 * wk.size)),
        )(x, gain.reshape(d // HEAD, HEAD), rate.reshape(1, HEAD), wq, wk, wv, wo)
        block = pl.BlockSpec((own // 4, d), lambda i: (i, 0))
        return pl.pallas_call(
            _copy,
            out_shape=jax.ShapeDtypeStruct((own, d), bf16),
            grid=(4,),
            in_specs=[block],
            out_specs=block,
        )(y)

    tokens, whole = P(("dp", "sp"), None), P(None, None)
    return jax.shard_map(
        step,
        mesh=mesh,
        in_specs=(tokens, P(None), whole, whole, whole, whole),
        out_specs=tokens,
        check_vma=False,
    )
```

```python
import functools

import jax
import jax.numpy as jnp
from jax import lax
from jax.experimental import pallas as pl
from jax.experimental.pallas import tpu as pltpu
from jax.sharding import PartitionSpec as P

HEAD = 128
THETA = 10000
HIDDEN = -2e30
LOG2E = 1.4426950408889634
DEPTH = 2048
WIDE = 512
SLOTS = 12
MESH = pl.DeviceIdType.MESH


def _dot(a, b, ca=1, cb=0):
    return lax.dot_general(a, b, (((ca,), (cb,)), ((), ())), preferred_element_type=jnp.float32)


def _kernel(n, x_hbm, gain_hbm, rate_hbm, wq, wk, wv, wo, y_hbm, x_s, a_s, ring, kv_s, q_s, acc_s, top_s, o_s, bias_s,
            raw_s, sum_s, s0_s, s1_s, p0_s, p1_s, t0_s, t1_s, r0_s, r1_s, gain_s, rate_s, cos_s, sin_s, x_sem, small_sem, y_sem, ring_sem, send_sem, recv_sem):
    own, d = x_s.shape
    heads, kv_heads = q_s.shape[0], kv_s.shape[2]
    group, half = heads // kv_heads, kv_heads // 2
    per = WIDE // HEAD
    e = HEAD**-0.5 * LOG2E
    me = lax.axis_index("sp")
    chips = n // 2
    core, chip = lax.rem(me, 2), lax.div(me, 2)
    right_chip, left_chip = lax.rem(chip + 1, chips), lax.rem(chip + chips - 1, chips)
    far_chip = lax.rem(chip + 2, chips)
    partner, right, left = chip * 2 + 1 - core, right_chip * 2 + core, left_chip * 2 + core

    rows = d // DEPTH
    o_rows = wo.shape[0] // DEPTH
    kv_chunks = kv_heads // per
    q_chunks, o_chunks = heads // per, wo.shape[1] // WIDE
    q_first = 2 * kv_chunks * rows
    o_first = q_first + q_chunks * rows
    ahead = SLOTS // rows
    reload = o_chunks - SLOTS // o_rows

    def fetch(src, part, chunk, slot):
        slot = slot % SLOTS if isinstance(slot, int) else lax.rem(slot, SLOTS)
        return pltpu.make_async_copy(src.at[pl.ds(part * DEPTH, DEPTH), pl.ds(chunk * WIDE, WIDE)], ring.at[slot], ring_sem.at[slot])

    def fetch_static(slot):
        if slot < q_first:
            c, part = slot // rows, slot % rows
            return fetch((wk, wv)[c % 2], part, c // 2, slot)
        c, part = (slot - q_first) // rows, (slot - q_first) % rows
        return fetch(wq, part, c, slot)

    def fetch_wq(c, part):
        return fetch(wq, part, c, q_first + rows * c + part)

    def fetch_wo(t):
        return fetch(wo, lax.rem(t, o_rows), lax.div(t, o_rows), o_first + t)

    def fetch_range(first, last):
        for slot in range(first, last):
            fetch_static(slot).start()

    x_copy = pltpu.make_async_copy(x_hbm, x_s, x_sem)
    x_copy.start()
    small = [pltpu.make_async_copy(gain_hbm, gain_s, small_sem.at[0]), pltpu.make_async_copy(rate_hbm, rate_s, small_sem.at[1])]
    for copy in small:
        copy.start()
    fetch_range(0, rows)

    barrier = pltpu.get_barrier_semaphore()
    for peer in (partner, right, left):
        pl.semaphore_signal(barrier, inc=1, device_id={"sp": peer}, device_id_type=MESH)

    def push_part(owner, h, slot, to, lane, part):
        ref = kv_s.at[owner, part, pl.ds(h * half, half)]
        return pltpu.make_async_remote_copy(ref, ref, send_sem.at[slot, lane, part], recv_sem.at[slot, lane, part], device_id={"sp": to},
                                            device_id_type=MESH)

    def push(owner, h, slot, to, lane):
        for part in range(2):
            push_part(owner, h, slot, to, lane, part).start()

    left_block, right_block, far_block = left_chip * 2 + core, right_chip * 2 + core, far_chip * 2 + core
    left_mate, right_mate, far_mate = left_chip * 2 + 1 - core, right_chip * 2 + 1 - core, far_chip * 2 + 1 - core

    for copy in small:
        copy.wait()
    angle = (me * own + lax.broadcasted_iota(jnp.int32, (own, HEAD), 0)).astype(jnp.float32) * rate_s[...]
    cos_s[...] = jnp.cos(angle)
    sin_s[...] = jnp.where(lax.broadcasted_iota(jnp.int32, (own, HEAD), 1) < HEAD // 2, -1.0, 1.0) * jnp.sin(angle)
    gain = jnp.concatenate([gain_s[i : i + 1, :].astype(jnp.float32) for i in range(d // HEAD)], axis=1)

    x_copy.wait()
    fetch_range(rows, 4 * rows)

    def norm(i, _):
        at = pl.ds(i * 32, 32)
        wide = x_s[at, :].astype(jnp.float32)
        scale = lax.rsqrt(jnp.mean(wide * wide, -1, keepdims=True) + 1e-6)
        a_s[at, :] = (wide * scale * gain).astype(jnp.bfloat16)
        return _

    lax.fori_loop(0, own // 32, norm, None)
    fetch_range(4 * rows, SLOTS)

    def slot_of(first, part):
        return (first + part) % SLOTS if isinstance(first, int) else lax.rem(first + part, SLOTS)

    def project(first, before):
        for part in range(rows):
            slot = slot_of(first, part)
            pltpu.make_async_copy(wq.at[pl.ds(0, DEPTH), pl.ds(0, WIDE)], ring.at[slot], ring_sem.at[slot]).wait()
        before()
        total = None
        for part in range(rows):
            term = _dot(a_s[:, part * DEPTH : (part + 1) * DEPTH], ring[slot_of(first, part)])
            total = term if total is None else total + term
        raw_s[...] = total.astype(jnp.bfloat16)

    def turned(i):
        t = raw_s[:, i * HEAD : (i + 1) * HEAD].astype(jnp.float32)
        return (t * cos_s[...] + pltpu.roll(t, HEAD // 2, 1) * sin_s[...]).astype(jnp.bfloat16)

    def keys(c):
        for i in range(per):
            kv_s[me, 0, c * per + i] = turned(i)

    def values(c):
        for i in range(per):
            for b in range(own // HEAD):
                kv_s[me, 1, c * per + i, b * HEAD : (b + 1) * HEAD, :] = raw_s[b * HEAD : (b + 1) * HEAD, i * HEAD : (i + 1) * HEAD].T

    def queries(c):
        for i in range(per):
            q_s[c * per + i] = turned(i)

    def kv(c, _):
        @pl.when(c == kv_chunks - 1)
        def _():
            pl.semaphore_wait(barrier, 3)
            push_part(me, 0, 1, right, 0, 0).start()

        project(2 * rows * c, lambda: values(jnp.maximum(c - 1, 0)))
        for part in range(rows):
            fetch_wq(2 * c + ahead - 2 * kv_chunks, part).start()

        @pl.when(c == kv_chunks - 1)
        def _():
            push_part(me, 0, 1, right, 0, 1).start()
            push(me, 0, 0, partner, 0)

        project(2 * rows * c + rows, lambda: keys(c))

        for part in range(rows):
            fetch_wq(2 * c + 1 + ahead - 2 * kv_chunks, part).start()
        return _

    lax.fori_loop(0, kv_chunks, kv, None)
    push_part(me, 1, 2, left, 1, 0).start()
    values(kv_chunks - 1)

    def query(c, _):
        project(q_first + rows * c, lambda: queries(jnp.maximum(c - 1, 0)))

        @pl.when(c == 0)
        def _():
            push_part(me, 1, 2, left, 1, 1).start()
            push(me, 1, 1, right, 1)
            push(me, 0, 2, left, 0)
            push(me, 1, 0, partner, 1)

        @pl.when(c < q_chunks - ahead)
        def _():
            for part in range(rows):
                fetch_wq(c + ahead, part).start()

        @pl.when(c >= q_chunks - ahead)
        def _():
            for part in range(rows):
                fetch_wo(rows * (c + ahead - q_chunks) + part).start()

        return _

    lax.fori_loop(0, q_chunks, query, None)
    queries(q_chunks - 1)

    span = 2 * own
    place = lax.broadcasted_iota(jnp.int32, (span, own), 1) - lax.broadcasted_iota(jnp.int32, (span, own), 0) + core * own
    bias_s[...] = jnp.where(place >= 0, 0.0, HIDDEN)
    pairs = group // 2
    units = half * pairs
    s_s, p_s, t_s, r_s = (s0_s, s1_s), (p0_s, p1_s), (t0_s, t1_s), (r0_s, r1_s)

    def attend(where, count, first, before=None):
        def scores(unit, slot):
            c, g, at = unit
            k = jnp.concatenate([kv_s[2 * c, 0, g], kv_s[2 * c + 1, 0, g]], axis=0)
            s = _dot(k, q_s[pl.ds(2 * at, 2)].reshape(2 * own, HEAD), 1, 1)
            if first:
                s = s + jnp.concatenate([bias_s[...], bias_s[...]], axis=1)
            s_s[slot][...] = s
            top = s.max(axis=0, keepdims=True)
            if not first:
                old = top_s[at]
                top = jnp.maximum(old, top)
                r_s[slot][...] = jnp.exp2((old - top) * e)
            top_s[at] = top
            t_s[slot][...] = top

        def weights(slot):
            for r in range(0, span, span // 8):
                at = slice(r, r + span // 8)
                p_s[slot][at, :] = jnp.exp2((s_s[slot][at, :] - t_s[slot][...]) * e).astype(jnp.bfloat16)

        def mix(unit, slot):
            c, g, at = unit
            squares = [kv_s[2 * c + i, 1, g, b * HEAD : (b + 1) * HEAD, :] for i in range(2) for b in range(own // HEAD)]
            v = jnp.concatenate([jnp.concatenate(squares, axis=1), jnp.ones((8, span), jnp.bfloat16)], axis=0)
            new = _dot(v, p_s[slot][...])
            acc_s[at] = new if first else acc_s[at] * r_s[slot][...] + new

        def body(i, _):
            if before is not None:
                before(i)
            held = [where(6 * i + k) for k in range(6 + 2)]
            for k in range(6):
                mix(held[k], k % 2)
                scores(held[k + 2], k % 2)
                weights(1 - k % 2)
            return _

        scores(where(0), 0)
        scores(where(1), 1)
        weights(0)
        lax.fori_loop(0, lax.div(count, 6) - 1, body, None)
        for k in range(6, 2, -1):
            mix(where(count - k), k % 2)
            scores(where(count - k + 2), k % 2)
            weights(1 - k % 2)
        mix(where(count - 2), 0)
        weights(1)
        mix(where(count - 1), 1)

    def arrive(owner, h, slot, lane):
        for part in range(2):
            push_part(owner, h, slot, me, lane, part).wait_recv()

    arrive(left_block, 0, 1, 0)
    push(left_block, 0, 3, right, 0)
    push(left_block, 0, 4, partner, 0)
    arrive(right_block, 1, 2, 1)
    push(right_block, 1, 3, left, 1)
    push(right_block, 1, 5, partner, 1)

    for h in range(2):
        arrive(partner, h, 0, h)
    attend(lambda u: (chip, lax.div(jnp.int32(u), pairs), jnp.int32(u)), chip * 0 + 2 * units, True)

    def seen(c):
        return jnp.where(c < chip, units, 0)

    begin1 = seen(left_chip) + seen(right_chip)
    begin2 = 2 * begin1
    count = begin2 + 2 * seen(far_chip)

    def round0():
        arrive(left_mate, 0, 4, 0)
        arrive(right_mate, 1, 5, 1)

    def round1():
        arrive(left_block, 1, 1, 1)
        push(left_block, 1, 4, partner, 1)
        arrive(right_block, 0, 2, 0)
        push(right_block, 0, 5, partner, 0)
        arrive(left_mate, 1, 4, 1)
        arrive(right_mate, 0, 5, 0)

    def round2():
        for h in range(2):
            arrive(far_block, h, 3, h)
            push(far_block, h, 6, partner, h)
        for h in range(2):
            arrive(far_mate, h, 6, h)

    def where(u):
        turn = jnp.where(u < begin1, 0, jnp.where(u < begin2, 1, 2))
        u = u - jnp.where(turn == 0, 0, jnp.where(turn == 1, begin1, begin2))
        second = lax.div(u, units)
        c = jnp.where(turn == 2, far_chip, jnp.where(second == 0, left_chip, right_chip))
        h = lax.rem(turn + second, 2)
        u = u - second * units
        at = h * units + u
        return c, lax.div(at, pairs), at

    def before(i):
        @pl.when(lax.div(begin1 - 2, 6) == i)
        def _():
            round1()

        @pl.when((lax.div(begin2 - 2, 6) == i) & (begin2 < count))
        def _():
            round2()

    round0()

    @pl.when(count > 0)
    def _():
        attend(where, count, False, before)

    @pl.when(count == 0)
    def _():
        round1()

    @pl.when(begin2 == count)
    def _():
        round2()

    def finish(first, _):
        for i in range(8):
            at = first * 4 + i // 2
            mixed = acc_s[at, :, i % 2 * own : (i % 2 + 1) * own]
            out = (mixed[:HEAD] * (1 / mixed[HEAD : HEAD + 1])).astype(jnp.bfloat16)
            o_s[:, pl.ds(pl.multiple_of((first * 8 + i) * HEAD, HEAD), HEAD)] = out.T
        return _

    lax.fori_loop(0, heads // 8, finish, None)

    def columns(c):
        return pl.ds(pl.multiple_of(c * WIDE, WIDE), WIDE)

    def result(c):
        return pltpu.make_async_copy(x_s.at[:, columns(c)], y_hbm.at[:, columns(c)], y_sem.at[c])

    def add(c):
        x_s[:, columns(c)] = (x_s[:, columns(c)].astype(jnp.float32) + sum_s[...]).astype(jnp.bfloat16)

    def out(c, _):
        for part in range(o_rows):
            fetch_wo(o_rows * c + part).wait()
        last = jnp.maximum(c - 1, 0)
        add(last)
        total = None
        for part in range(o_rows):
            term = _dot(o_s[:, part * DEPTH : (part + 1) * DEPTH], ring[lax.rem(o_first + o_rows * c + part, SLOTS)])
            total = term if total is None else total + term
        sum_s[...] = total

        @pl.when(c < reload)
        def _():
            for part in range(o_rows):
                fetch_wo(o_rows * c + part + SLOTS).start()

        @pl.when(c > 0)
        def _():
            result(last).start()

        return _

    sum_s[...] = jnp.zeros_like(sum_s)
    lax.fori_loop(0, o_chunks, out, None)
    add(o_chunks - 1)
    result(o_chunks - 1).start()
    for c in range(o_chunks):
        result(c).wait()

    for h in range(2):
        for slot in range(7):
            for part in range(2):
                push_part(me, h, slot, partner, h, part).wait_send()


def _copy(a_hbm, b_hbm, held, sem):
    rows = a_hbm.shape[0] // 8
    reads = [pltpu.make_async_copy(a_hbm.at[pl.ds(i * rows, rows)], held.at[pl.ds(i * rows, rows)], sem.at[0, i]) for i in range(8)]
    writes = [pltpu.make_async_copy(held.at[pl.ds(i * rows, rows)], b_hbm.at[pl.ds(i * rows, rows)], sem.at[1, i]) for i in range(8)]
    for read in reads:
        read.start()
    for read, write in zip(reads, writes):
        read.wait()
        write.start()
    for write in writes:
        write.wait()


def solution(mesh):
    n = mesh.shape["sp"]

    def step(x, gain, wq, wk, wv, wo):
        own, d = x.shape
        heads, kv_heads = wq.shape[1] // HEAD, wk.shape[1] // HEAD
        half = HEAD // 2
        rate = THETA ** (-(jnp.arange(HEAD) % half).astype(jnp.float32) / half)
        anywhere = pl.BlockSpec(memory_space=pl.ANY)
        bf16, f32 = jnp.bfloat16, jnp.float32
        pairs, span = heads // 2, 2 * own
        y = pl.pallas_call(
            functools.partial(_kernel, n),
            out_shape=jax.ShapeDtypeStruct((own, d), bf16),
            in_specs=[anywhere] * 7,
            out_specs=anywhere,
            scratch_shapes=[
                pltpu.VMEM((own, d), bf16),
                pltpu.VMEM((own, d), bf16),
                pltpu.VMEM((SLOTS, DEPTH, WIDE), bf16),
                pltpu.VMEM((n, 2, kv_heads, own, HEAD), bf16),
                pltpu.VMEM((heads, own, HEAD), bf16),
                pltpu.VMEM((pairs, HEAD + 8, span), f32),
                pltpu.VMEM((pairs, 1, span), f32),
                pltpu.VMEM((own, heads * HEAD), bf16),
                pltpu.VMEM((span, own), f32),
                pltpu.VMEM((own, WIDE), bf16),
                pltpu.VMEM((own, WIDE), f32),
                pltpu.VMEM((span, span), f32),
                pltpu.VMEM((span, span), f32),
                pltpu.VMEM((span, span), bf16),
                pltpu.VMEM((span, span), bf16),
                pltpu.VMEM((1, span), f32),
                pltpu.VMEM((1, span), f32),
                pltpu.VMEM((1, span), f32),
                pltpu.VMEM((1, span), f32),
                pltpu.VMEM((d // HEAD, HEAD), bf16),
                pltpu.VMEM((1, HEAD), f32),
                pltpu.VMEM((own, HEAD), f32),
                pltpu.VMEM((own, HEAD), f32),
                pltpu.SemaphoreType.DMA,
                pltpu.SemaphoreType.DMA((2,)),
                pltpu.SemaphoreType.DMA((wo.shape[1] // WIDE,)),
                pltpu.SemaphoreType.DMA((SLOTS,)),
                pltpu.SemaphoreType.DMA((7, 2, 2)),
                pltpu.SemaphoreType.DMA((7, 2, 2)),
            ],
            compiler_params=pltpu.CompilerParams(collective_id=0, has_side_effects=True, vmem_limit_bytes=67043328),
            cost_estimate=pl.CostEstimate(flops=2 * own * d * (2 * wq.shape[1] + 2 * wk.shape[1]), transcendentals=heads * own * own * n,
                                          bytes_accessed=2 * (2 * wq.size + 2 * wk.size)),
        )(x, gain.reshape(d // HEAD, HEAD), rate.reshape(1, HEAD), wq, wk, wv, wo)
        return pl.pallas_call(
            _copy,
            out_shape=jax.ShapeDtypeStruct((own, d), bf16),
            in_specs=[anywhere],
            out_specs=anywhere,
            scratch_shapes=[pltpu.VMEM((own, d), bf16), pltpu.SemaphoreType.DMA((2, 8))],
        )(y)

    tokens, whole = P(("dp", "sp"), None), P(None, None)
    return jax.shard_map(
        step,
        mesh=mesh,
        in_specs=(tokens, P(None), whole, whole, whole, whole),
        out_specs=tokens,
        check_vma=False,
    )
```

```python
import functools

import jax
import jax.numpy as jnp
import numpy as np
from jax import lax
from jax.experimental import pallas as pl
from jax.experimental.pallas import tpu as pltpu
from jax.sharding import PartitionSpec as P

HEAD = 128
THETA = 10000
HIDDEN = -2e30
LOG2E = 1.4426950408889634
DEPTH = 2048
WIDE = 512
SLOTS = 12
MESH = pl.DeviceIdType.MESH


def _dot(a, b, ca=1, cb=0):
    return lax.dot_general(a, b, (((ca,), (cb,)), ((), ())), preferred_element_type=jnp.float32)


def _kernel(n, x_hbm, gain_hbm, rate_hbm, wq, wk, wv, wo, y_hbm, x_s, a_s, ring, kv_s, q_s, acc_s, top_s, o_s, bias_s,
            raw_s, sum_s, s0_s, s1_s, p0_s, p1_s, t0_s, t1_s, r0_s, r1_s, gain_s, rate_s, cos_s, sin_s, x_sem, small_sem, y_sem, ring_sem, send_sem, recv_sem):
    own, d = x_s.shape
    heads, kv_heads = q_s.shape[0], kv_s.shape[2]
    group, half = heads // kv_heads, kv_heads // 2
    per = WIDE // HEAD
    e = HEAD**-0.5 * LOG2E
    me = lax.axis_index("sp")
    chips = n // 2
    core, chip = lax.rem(me, 2), lax.div(me, 2)
    right_chip, left_chip = lax.rem(chip + 1, chips), lax.rem(chip + chips - 1, chips)
    far_chip = lax.rem(chip + 2, chips)
    partner, right, left = chip * 2 + 1 - core, right_chip * 2 + core, left_chip * 2 + core

    rows = d // DEPTH
    o_rows = wo.shape[0] // DEPTH
    kv_chunks = kv_heads // per
    q_chunks, o_chunks = heads // per, wo.shape[1] // WIDE
    q_first = 2 * kv_chunks * rows
    o_first = q_first + q_chunks * rows
    ahead = SLOTS // rows
    reload = o_chunks - SLOTS // o_rows

    def fetch(src, part, chunk, slot):
        slot = slot % SLOTS if isinstance(slot, int) else lax.rem(slot, SLOTS)
        return pltpu.make_async_copy(src.at[pl.ds(part * DEPTH, DEPTH), pl.ds(chunk * WIDE, WIDE)], ring.at[slot], ring_sem.at[slot])

    def fetch_static(slot):
        if slot < q_first:
            c, part = slot // rows, slot % rows
            return fetch((wk, wv)[c % 2], part, c // 2, slot)
        c, part = (slot - q_first) // rows, (slot - q_first) % rows
        return fetch(wq, part, c, slot)

    def fetch_wq(c, part):
        return fetch(wq, part, c, q_first + rows * c + part)

    def fetch_wo(t):
        return fetch(wo, lax.rem(t, o_rows), lax.div(t, o_rows), o_first + t)

    def fetch_range(first, last):
        for slot in range(first, last):
            fetch_static(slot).start()

    x_copy = pltpu.make_async_copy(x_hbm, x_s, x_sem)
    x_copy.start()
    small = [pltpu.make_async_copy(gain_hbm, gain_s, small_sem.at[0]), pltpu.make_async_copy(rate_hbm, rate_s, small_sem.at[1])]
    for copy in small:
        copy.start()
    fetch_range(0, rows)

    barrier = pltpu.get_barrier_semaphore()
    for peer in (partner, right, left):
        pl.semaphore_signal(barrier, inc=1, device_id={"sp": peer}, device_id_type=MESH)

    def push_part(owner, h, slot, to, lane, part):
        ref = kv_s.at[owner, part, pl.ds(h * half, half)]
        return pltpu.make_async_remote_copy(ref, ref, send_sem.at[slot, lane, part], recv_sem.at[slot, lane, part], device_id={"sp": to},
                                            device_id_type=MESH)

    def push(owner, h, slot, to, lane):
        for part in range(2):
            push_part(owner, h, slot, to, lane, part).start()

    left_block, right_block, far_block = left_chip * 2 + core, right_chip * 2 + core, far_chip * 2 + core
    left_mate, right_mate, far_mate = left_chip * 2 + 1 - core, right_chip * 2 + 1 - core, far_chip * 2 + 1 - core

    for copy in small:
        copy.wait()
    angle = (me * own + lax.broadcasted_iota(jnp.int32, (own, HEAD), 0)).astype(jnp.float32) * rate_s[...]
    cos_s[...] = jnp.cos(angle)
    sin_s[...] = jnp.where(lax.broadcasted_iota(jnp.int32, (own, HEAD), 1) < HEAD // 2, -1.0, 1.0) * jnp.sin(angle)
    gain = jnp.concatenate([gain_s[i : i + 1, :].astype(jnp.float32) for i in range(d // HEAD)], axis=1)

    x_copy.wait()
    fetch_range(rows, 4 * rows)

    def norm(i, _):
        at = pl.ds(i * 32, 32)
        wide = x_s[at, :].astype(jnp.float32)
        scale = lax.rsqrt(jnp.mean(wide * wide, -1, keepdims=True) + 1e-6)
        a_s[at, :] = (wide * scale * gain).astype(jnp.bfloat16)
        return _

    lax.fori_loop(0, own // 32, norm, None)
    fetch_range(4 * rows, SLOTS)

    def slot_of(first, part):
        return (first + part) % SLOTS if isinstance(first, int) else lax.rem(first + part, SLOTS)

    def project(first, before):
        for part in range(rows):
            slot = slot_of(first, part)
            pltpu.make_async_copy(wq.at[pl.ds(0, DEPTH), pl.ds(0, WIDE)], ring.at[slot], ring_sem.at[slot]).wait()
        before()
        total = None
        for part in range(rows):
            term = _dot(a_s[:, part * DEPTH : (part + 1) * DEPTH], ring[slot_of(first, part)])
            total = term if total is None else total + term
        raw_s[...] = total.astype(jnp.bfloat16)

    def turned(i):
        t = raw_s[:, i * HEAD : (i + 1) * HEAD].astype(jnp.float32)
        return (t * cos_s[...] + pltpu.roll(t, HEAD // 2, 1) * sin_s[...]).astype(jnp.bfloat16)

    def keys(c):
        for i in range(per):
            kv_s[me, 0, c * per + i] = turned(i)

    def values(c):
        for i in range(per):
            for b in range(own // HEAD):
                kv_s[me, 1, c * per + i, b * HEAD : (b + 1) * HEAD, :] = raw_s[b * HEAD : (b + 1) * HEAD, i * HEAD : (i + 1) * HEAD].T

    def queries(c):
        for i in range(per):
            q_s[c * per + i] = turned(i)

    def kv(c, _):
        @pl.when(c == kv_chunks - 1)
        def _():
            pl.semaphore_wait(barrier, 3)
            push_part(me, 0, 1, right, 0, 0).start()

        project(2 * rows * c, lambda: values(jnp.maximum(c - 1, 0)))
        for part in range(rows):
            fetch_wq(2 * c + ahead - 2 * kv_chunks, part).start()

        @pl.when(c == kv_chunks - 1)
        def _():
            push_part(me, 0, 1, right, 0, 1).start()

        project(2 * rows * c + rows, lambda: keys(c))

        for part in range(rows):
            fetch_wq(2 * c + 1 + ahead - 2 * kv_chunks, part).start()
        return _

    lax.fori_loop(0, kv_chunks, kv, None)
    push_part(me, 1, 2, left, 1, 0).start()
    values(kv_chunks - 1)

    def query(c, _):
        project(q_first + rows * c, lambda: queries(jnp.maximum(c - 1, 0)))

        sends = {
            q_chunks // 4: [(1, 2, left, 1, 1)],
            q_chunks // 4 + 1: [(1, 1, right, 1, 0)],
            q_chunks // 2: [(0, 2, left, 0, 0), (0, 0, partner, 0, 0), (0, 0, partner, 0, 1)],
            q_chunks // 2 + 2: [(1, 1, right, 1, 1), (1, 0, partner, 1, 0), (1, 0, partner, 1, 1)],
            q_chunks - 3: [(0, 2, left, 0, 1)],
        }
        for when, parts in sends.items():

            @pl.when(c == when)
            def _():
                for h, slot, to, lane, part in parts:
                    push_part(me, h, slot, to, lane, part).start()

        @pl.when(c < q_chunks - ahead)
        def _():
            for part in range(rows):
                fetch_wq(c + ahead, part).start()

        @pl.when(c >= q_chunks - ahead)
        def _():
            for part in range(rows):
                fetch_wo(rows * (c + ahead - q_chunks) + part).start()

        return _

    lax.fori_loop(0, q_chunks, query, None)
    queries(q_chunks - 1)

    span = 2 * own
    place = lax.broadcasted_iota(jnp.int32, (span, own), 1) - lax.broadcasted_iota(jnp.int32, (span, own), 0) + core * own
    bias_s[...] = jnp.where(place >= 0, 0.0, HIDDEN)
    pairs = group // 2
    units = half * pairs
    s_s, p_s, t_s, r_s = (s0_s, s1_s), (p0_s, p1_s), (t0_s, t1_s), (r0_s, r1_s)

    def attend(where, count, first, before=None):
        def scores(unit, slot):
            c, g, at = unit
            k = jnp.concatenate([kv_s[2 * c, 0, g], kv_s[2 * c + 1, 0, g]], axis=0)
            s = _dot(k, q_s[pl.ds(2 * at, 2)].reshape(2 * own, HEAD), 1, 1)
            if first:
                s = s + jnp.concatenate([bias_s[...], bias_s[...]], axis=1)
            s_s[slot][...] = s
            top = s.max(axis=0, keepdims=True)
            if not first:
                old = top_s[at]
                top = jnp.maximum(old, top)
                r_s[slot][...] = jnp.exp2((old - top) * e)
            top_s[at] = top
            t_s[slot][...] = top

        def weights(slot):
            for r in range(0, span, span // 8):
                at = slice(r, r + span // 8)
                p_s[slot][at, :] = jnp.exp2((s_s[slot][at, :] - t_s[slot][...]) * e).astype(jnp.bfloat16)

        def mix(unit, slot):
            c, g, at = unit
            squares = [kv_s[2 * c + i, 1, g, b * HEAD : (b + 1) * HEAD, :] for i in range(2) for b in range(own // HEAD)]
            v = jnp.concatenate([jnp.concatenate(squares, axis=1), jnp.ones((8, span), jnp.bfloat16)], axis=0)
            new = _dot(v, p_s[slot][...])
            acc_s[at] = new if first else acc_s[at] * r_s[slot][...] + new

        def body(i, _):
            if before is not None:
                before(i)
            held = [where(6 * i + k) for k in range(6 + 2)]
            for k in range(6):
                mix(held[k], k % 2)
                scores(held[k + 2], k % 2)
                weights(1 - k % 2)
            return _

        scores(where(0), 0)
        scores(where(1), 1)
        weights(0)
        lax.fori_loop(0, lax.div(count, 6) - 1, body, None)
        for k in range(6, 2, -1):
            mix(where(count - k), k % 2)
            scores(where(count - k + 2), k % 2)
            weights(1 - k % 2)
        mix(where(count - 2), 0)
        weights(1)
        mix(where(count - 1), 1)

    def arrive(owner, h, slot, lane):
        for part in range(2):
            push_part(owner, h, slot, me, lane, part).wait_recv()

    arrive(left_block, 0, 1, 0)
    push(left_block, 0, 3, right, 0)
    push(left_block, 0, 4, partner, 0)
    arrive(right_block, 1, 2, 1)
    push(right_block, 1, 3, left, 1)
    push(right_block, 1, 5, partner, 1)

    for h in range(2):
        arrive(partner, h, 0, h)
    attend(lambda u: (chip, lax.div(jnp.int32(u), pairs), jnp.int32(u)), chip * 0 + 2 * units, True)

    def seen(c):
        return jnp.where(c < chip, units, 0)

    begin1 = seen(left_chip) + seen(right_chip)
    begin2 = 2 * begin1
    count = begin2 + 2 * seen(far_chip)

    def round0():
        arrive(left_mate, 0, 4, 0)
        arrive(right_mate, 1, 5, 1)

    def round1():
        arrive(left_block, 1, 1, 1)
        push(left_block, 1, 4, partner, 1)
        arrive(right_block, 0, 2, 0)
        push(right_block, 0, 5, partner, 0)
        arrive(left_mate, 1, 4, 1)
        arrive(right_mate, 0, 5, 0)

    def round2():
        for h in range(2):
            arrive(far_block, h, 3, h)
            push(far_block, h, 6, partner, h)
        for h in range(2):
            arrive(far_mate, h, 6, h)

    def where(u):
        turn = jnp.where(u < begin1, 0, jnp.where(u < begin2, 1, 2))
        u = u - jnp.where(turn == 0, 0, jnp.where(turn == 1, begin1, begin2))
        second = lax.div(u, units)
        c = jnp.where(turn == 2, far_chip, jnp.where(second == 0, left_chip, right_chip))
        h = lax.rem(turn + second, 2)
        u = u - second * units
        at = h * units + u
        return c, lax.div(at, pairs), at

    def before(i):
        @pl.when(lax.div(begin1 - 2, 6) == i)
        def _():
            round1()

        @pl.when((lax.div(begin2 - 2, 6) == i) & (begin2 < count))
        def _():
            round2()

    round0()

    @pl.when(count > 0)
    def _():
        attend(where, count, False, before)

    @pl.when(count == 0)
    def _():
        round1()

    @pl.when(begin2 == count)
    def _():
        round2()

    def finish(first, _):
        for i in range(8):
            at = first * 4 + i // 2
            mixed = acc_s[at, :, i % 2 * own : (i % 2 + 1) * own]
            out = (mixed[:HEAD] * (1 / mixed[HEAD : HEAD + 1])).astype(jnp.bfloat16)
            o_s[:, pl.ds(pl.multiple_of((first * 8 + i) * HEAD, HEAD), HEAD)] = out.T
        return _

    lax.fori_loop(0, heads // 8, finish, None)

    def columns(c):
        return pl.ds(pl.multiple_of(c * WIDE, WIDE), WIDE)

    def result(c):
        return pltpu.make_async_copy(x_s.at[:, columns(c)], y_hbm.at[:, columns(c)], y_sem.at[c])

    def add(c):
        x_s[:, columns(c)] = (x_s[:, columns(c)].astype(jnp.float32) + sum_s[...]).astype(jnp.bfloat16)

    def out(c, _):
        for part in range(o_rows):
            fetch_wo(o_rows * c + part).wait()
        last = jnp.maximum(c - 1, 0)
        add(last)
        total = None
        for part in range(o_rows):
            term = _dot(o_s[:, part * DEPTH : (part + 1) * DEPTH], ring[lax.rem(o_first + o_rows * c + part, SLOTS)])
            total = term if total is None else total + term
        sum_s[...] = total

        @pl.when(c < reload)
        def _():
            for part in range(o_rows):
                fetch_wo(o_rows * c + part + SLOTS).start()

        @pl.when(c > 0)
        def _():
            result(last).start()

        return _

    sum_s[...] = jnp.zeros_like(sum_s)
    lax.fori_loop(0, o_chunks, out, None)
    add(o_chunks - 1)
    result(o_chunks - 1).start()
    for c in range(o_chunks):
        result(c).wait()

    for h in range(2):
        for slot in range(7):
            for part in range(2):
                push_part(me, h, slot, partner, h, part).wait_send()


def _copy(a_hbm, b_hbm, held, sem):
    rows = a_hbm.shape[0] // 8
    reads = [pltpu.make_async_copy(a_hbm.at[pl.ds(i * rows, rows)], held.at[pl.ds(i * rows, rows)], sem.at[0, i]) for i in range(8)]
    writes = [pltpu.make_async_copy(held.at[pl.ds(i * rows, rows)], b_hbm.at[pl.ds(i * rows, rows)], sem.at[1, i]) for i in range(8)]
    for read in reads:
        read.start()
    for read, write in zip(reads, writes):
        read.wait()
        write.start()
    for write in writes:
        write.wait()


def solution(mesh):
    n = mesh.shape["sp"]

    def step(x, gain, wq, wk, wv, wo):
        own, d = x.shape
        heads, kv_heads = wq.shape[1] // HEAD, wk.shape[1] // HEAD
        half = HEAD // 2
        rate = np.float32(THETA) ** (-(np.arange(HEAD) % half).astype(np.float32) / half)
        anywhere = pl.BlockSpec(memory_space=pl.ANY)
        bf16, f32 = jnp.bfloat16, jnp.float32
        pairs, span = heads // 2, 2 * own
        y = pl.pallas_call(
            functools.partial(_kernel, n),
            out_shape=jax.ShapeDtypeStruct((own, d), bf16),
            in_specs=[anywhere] * 7,
            out_specs=anywhere,
            scratch_shapes=[
                pltpu.VMEM((own, d), bf16),
                pltpu.VMEM((own, d), bf16),
                pltpu.VMEM((SLOTS, DEPTH, WIDE), bf16),
                pltpu.VMEM((n, 2, kv_heads, own, HEAD), bf16),
                pltpu.VMEM((heads, own, HEAD), bf16),
                pltpu.VMEM((pairs, HEAD + 8, span), f32),
                pltpu.VMEM((pairs, 1, span), f32),
                pltpu.VMEM((own, heads * HEAD), bf16),
                pltpu.VMEM((span, own), f32),
                pltpu.VMEM((own, WIDE), bf16),
                pltpu.VMEM((own, WIDE), f32),
                pltpu.VMEM((span, span), f32),
                pltpu.VMEM((span, span), f32),
                pltpu.VMEM((span, span), bf16),
                pltpu.VMEM((span, span), bf16),
                pltpu.VMEM((1, span), f32),
                pltpu.VMEM((1, span), f32),
                pltpu.VMEM((1, span), f32),
                pltpu.VMEM((1, span), f32),
                pltpu.VMEM((d // HEAD, HEAD), bf16),
                pltpu.VMEM((1, HEAD), f32),
                pltpu.VMEM((own, HEAD), f32),
                pltpu.VMEM((own, HEAD), f32),
                pltpu.SemaphoreType.DMA,
                pltpu.SemaphoreType.DMA((2,)),
                pltpu.SemaphoreType.DMA((wo.shape[1] // WIDE,)),
                pltpu.SemaphoreType.DMA((SLOTS,)),
                pltpu.SemaphoreType.DMA((7, 2, 2)),
                pltpu.SemaphoreType.DMA((7, 2, 2)),
            ],
            compiler_params=pltpu.CompilerParams(collective_id=0, has_side_effects=True, vmem_limit_bytes=67043328),
            cost_estimate=pl.CostEstimate(flops=2 * own * d * (2 * wq.shape[1] + 2 * wk.shape[1]), transcendentals=heads * own * own * n,
                                          bytes_accessed=2 * (2 * wq.size + 2 * wk.size)),
        )(x, gain.reshape(d // HEAD, HEAD), jnp.asarray(rate, f32).reshape(1, HEAD), wq, wk, wv, wo)
        return pl.pallas_call(
            _copy,
            out_shape=jax.ShapeDtypeStruct((own, d), bf16),
            in_specs=[anywhere],
            out_specs=anywhere,
            scratch_shapes=[pltpu.VMEM((own, d), bf16), pltpu.SemaphoreType.DMA((2, 8))],
        )(y)

    tokens, whole = P(("dp", "sp"), None), P(None, None)
    return jax.shard_map(
        step,
        mesh=mesh,
        in_specs=(tokens, P(None), whole, whole, whole, whole),
        out_specs=tokens,
        check_vma=False,
    )
```

```python
import functools

import jax
import jax.numpy as jnp
import numpy as np
from jax import lax
from jax.experimental import pallas as pl
from jax.experimental.pallas import tpu as pltpu
from jax.sharding import PartitionSpec as P

HEAD = 128
THETA = 10000
HIDDEN = -2e30
LOG2E = 1.4426950408889634
DEPTH = 2048
WIDE = 512
SLOTS = 12
MESH = pl.DeviceIdType.MESH


def _dot(a, b, ca=1, cb=0):
    return lax.dot_general(a, b, (((ca,), (cb,)), ((), ())), preferred_element_type=jnp.float32)


def _kernel(n, x_hbm, gain_hbm, rate_hbm, wq, wk, wv, wo, y_hbm, x_s, a_s, ring, kv_s, q_s, acc_s, top_s, o_s, bias_s,
            raw_s, sum_s, s0_s, s1_s, p0_s, p1_s, t0_s, t1_s, r0_s, r1_s, gain_s, rate_s, cos_s, sin_s, x_sem, small_sem, y_sem, ring_sem, send_sem, recv_sem):
    own, d = x_s.shape
    heads, kv_heads = q_s.shape[0], kv_s.shape[2]
    group, half = heads // kv_heads, kv_heads // 2
    per = WIDE // HEAD
    e = HEAD**-0.5 * LOG2E
    me = lax.axis_index("sp")
    chips = n // 2
    core, chip = lax.rem(me, 2), lax.div(me, 2)
    right_chip, left_chip = lax.rem(chip + 1, chips), lax.rem(chip + chips - 1, chips)
    far_chip = lax.rem(chip + 2, chips)
    partner, right, left = chip * 2 + 1 - core, right_chip * 2 + core, left_chip * 2 + core

    rows = d // DEPTH
    o_rows = wo.shape[0] // DEPTH
    kv_chunks = kv_heads // per
    q_chunks, o_chunks = heads // per, wo.shape[1] // WIDE
    q_first = 2 * kv_chunks * rows
    o_first = q_first + q_chunks * rows
    ahead = SLOTS // rows
    reload = o_chunks - SLOTS // o_rows

    def fetch(src, part, chunk, slot):
        slot = slot % SLOTS if isinstance(slot, int) else lax.rem(slot, SLOTS)
        return pltpu.make_async_copy(src.at[pl.ds(part * DEPTH, DEPTH), pl.ds(chunk * WIDE, WIDE)], ring.at[slot], ring_sem.at[slot])

    def fetch_static(slot):
        if slot < q_first:
            c, part = slot // rows, slot % rows
            return fetch((wk, wv)[c % 2], part, c // 2, slot)
        c, part = (slot - q_first) // rows, (slot - q_first) % rows
        return fetch(wq, part, c, slot)

    def fetch_wq(c, part):
        return fetch(wq, part, c, q_first + rows * c + part)

    def fetch_wo(t):
        return fetch(wo, lax.rem(t, o_rows), lax.div(t, o_rows), o_first + t)

    def fetch_range(first, last):
        for slot in range(first, last):
            fetch_static(slot).start()

    x_copy = pltpu.make_async_copy(x_hbm, x_s, x_sem)
    x_copy.start()
    small = [pltpu.make_async_copy(gain_hbm, gain_s, small_sem.at[0]), pltpu.make_async_copy(rate_hbm, rate_s, small_sem.at[1])]
    for copy in small:
        copy.start()
    fetch_range(0, rows)

    barrier = pltpu.get_barrier_semaphore()
    for peer in (partner, right, left):
        pl.semaphore_signal(barrier, inc=1, device_id={"sp": peer}, device_id_type=MESH)

    def push_part(owner, h, slot, to, lane, part):
        ref = kv_s.at[owner, part, pl.ds(h * half, half)]
        return pltpu.make_async_remote_copy(ref, ref, send_sem.at[slot, lane, part], recv_sem.at[slot, lane, part], device_id={"sp": to},
                                            device_id_type=MESH)

    def push(owner, h, slot, to, lane):
        for part in range(2):
            push_part(owner, h, slot, to, lane, part).start()

    left_block, right_block, far_block = left_chip * 2 + core, right_chip * 2 + core, far_chip * 2 + core
    left_mate, right_mate, far_mate = left_chip * 2 + 1 - core, right_chip * 2 + 1 - core, far_chip * 2 + 1 - core

    for copy in small:
        copy.wait()
    angle = (me * own + lax.broadcasted_iota(jnp.int32, (own, HEAD), 0)).astype(jnp.float32) * rate_s[...]
    cos_s[...] = jnp.cos(angle)
    sin_s[...] = jnp.where(lax.broadcasted_iota(jnp.int32, (own, HEAD), 1) < HEAD // 2, -1.0, 1.0) * jnp.sin(angle)
    gain = jnp.concatenate([gain_s[i : i + 1, :].astype(jnp.float32) for i in range(d // HEAD)], axis=1)

    x_copy.wait()
    fetch_range(rows, 4 * rows)

    def norm(i, _):
        at = pl.ds(i * 32, 32)
        wide = x_s[at, :].astype(jnp.float32)
        scale = lax.rsqrt(jnp.mean(wide * wide, -1, keepdims=True) + 1e-6)
        a_s[at, :] = (wide * scale * gain).astype(jnp.bfloat16)
        return _

    lax.fori_loop(0, own // 32, norm, None, unroll=2)
    fetch_range(4 * rows, SLOTS)

    def slot_of(first, part):
        return (first + part) % SLOTS if isinstance(first, int) else lax.rem(first + part, SLOTS)

    def project(first, before):
        for part in range(rows):
            slot = slot_of(first, part)
            pltpu.make_async_copy(wq.at[pl.ds(0, DEPTH), pl.ds(0, WIDE)], ring.at[slot], ring_sem.at[slot]).wait()
        before()
        total = None
        for part in range(rows):
            term = _dot(a_s[:, part * DEPTH : (part + 1) * DEPTH], ring[slot_of(first, part)])
            total = term if total is None else total + term
        raw_s[...] = total.astype(jnp.bfloat16)

    def turned(i):
        t = raw_s[:, i * HEAD : (i + 1) * HEAD].astype(jnp.float32)
        return t * cos_s[...] + pltpu.roll(t, HEAD // 2, 1) * sin_s[...]

    def keys(c):
        for i in range(per):
            kv_s[me, 0, c * per + i] = turned(i).astype(jnp.bfloat16)

    def values(c):
        for i in range(per):
            for b in range(own // HEAD):
                kv_s[me, 1, c * per + i, b * HEAD : (b + 1) * HEAD, :] = raw_s[b * HEAD : (b + 1) * HEAD, i * HEAD : (i + 1) * HEAD].T

    def queries(c):
        for i in range(per):
            q_s[c * per + i] = (turned(i) * e).astype(jnp.bfloat16)

    def kv(c, _):
        @pl.when(c == kv_chunks - 1)
        def _():
            pl.semaphore_wait(barrier, 3)
            push_part(me, 0, 1, right, 0, 0).start()

        project(2 * rows * c, lambda: values(jnp.maximum(c - 1, 0)))
        for part in range(rows):
            fetch_wq(2 * c + ahead - 2 * kv_chunks, part).start()

        @pl.when(c == kv_chunks - 1)
        def _():
            push_part(me, 0, 1, right, 0, 1).start()

        project(2 * rows * c + rows, lambda: keys(c))

        for part in range(rows):
            fetch_wq(2 * c + 1 + ahead - 2 * kv_chunks, part).start()
        return _

    lax.fori_loop(0, kv_chunks, kv, None)
    push_part(me, 1, 2, left, 1, 0).start()
    values(kv_chunks - 1)

    def query(c, _):
        project(q_first + rows * c, lambda: queries(jnp.maximum(c - 1, 0)))

        sends = {
            q_chunks // 4: [(1, 2, left, 1, 1)],
            q_chunks // 4 + 1: [(1, 1, right, 1, 0)],
            q_chunks // 2: [(0, 2, left, 0, 0), (0, 0, partner, 0, 0), (0, 0, partner, 0, 1)],
            q_chunks // 2 + 2: [(1, 1, right, 1, 1), (1, 0, partner, 1, 0), (1, 0, partner, 1, 1)],
            q_chunks - 3: [(0, 2, left, 0, 1)],
        }
        for when, parts in sends.items():

            @pl.when(c == when)
            def _():
                for h, slot, to, lane, part in parts:
                    push_part(me, h, slot, to, lane, part).start()

        @pl.when(c < q_chunks - ahead)
        def _():
            for part in range(rows):
                fetch_wq(c + ahead, part).start()

        @pl.when(c >= q_chunks - ahead)
        def _():
            for part in range(rows):
                fetch_wo(rows * (c + ahead - q_chunks) + part).start()

        return _

    lax.fori_loop(0, q_chunks, query, None)
    queries(q_chunks - 1)

    span = 2 * own
    place = lax.broadcasted_iota(jnp.int32, (span, own), 1) - lax.broadcasted_iota(jnp.int32, (span, own), 0) + core * own
    bias_s[...] = jnp.where(place >= 0, 0.0, HIDDEN)
    pairs = group // 2
    units = half * pairs
    s_s, p_s, t_s, r_s = (s0_s, s1_s), (p0_s, p1_s), (t0_s, t1_s), (r0_s, r1_s)

    def attend(where, count, first, before=None):
        def scores(unit, slot):
            c, g, at = unit
            k = jnp.concatenate([kv_s[2 * c, 0, g], kv_s[2 * c + 1, 0, g]], axis=0)
            s = _dot(k, q_s[pl.ds(2 * at, 2)].reshape(2 * own, HEAD), 1, 1)
            if first:
                s = s + jnp.concatenate([bias_s[...], bias_s[...]], axis=1)
            s_s[slot][...] = s
            top = s.max(axis=0, keepdims=True)
            if not first:
                old = top_s[at]
                top = jnp.maximum(old, top)
                r_s[slot][...] = jnp.exp2(old - top)
            top_s[at] = top
            t_s[slot][...] = top

        def weights(slot):
            for r in range(0, span, span // 8):
                at = slice(r, r + span // 8)
                p_s[slot][at, :] = jnp.exp2(s_s[slot][at, :] - t_s[slot][...]).astype(jnp.bfloat16)

        def mix(unit, slot):
            c, g, at = unit
            squares = [kv_s[2 * c + i, 1, g, b * HEAD : (b + 1) * HEAD, :] for i in range(2) for b in range(own // HEAD)]
            v = jnp.concatenate([jnp.concatenate(squares, axis=1), jnp.ones((8, span), jnp.bfloat16)], axis=0)
            new = _dot(v, p_s[slot][...])
            acc_s[at] = new if first else acc_s[at] * r_s[slot][...] + new

        def body(i, _):
            if before is not None:
                before(i)
            held = [where(6 * i + k) for k in range(6 + 2)]
            for k in range(6):
                mix(held[k], k % 2)
                scores(held[k + 2], k % 2)
                weights(1 - k % 2)
            return _

        scores(where(0), 0)
        scores(where(1), 1)
        weights(0)
        lax.fori_loop(0, lax.div(count, 6) - 1, body, None)
        for k in range(6, 2, -1):
            mix(where(count - k), k % 2)
            scores(where(count - k + 2), k % 2)
            weights(1 - k % 2)
        mix(where(count - 2), 0)
        weights(1)
        mix(where(count - 1), 1)

    def arrive(owner, h, slot, lane):
        for part in range(2):
            push_part(owner, h, slot, me, lane, part).wait_recv()

    arrive(left_block, 0, 1, 0)
    push(left_block, 0, 3, right, 0)
    push(left_block, 0, 4, partner, 0)
    arrive(right_block, 1, 2, 1)
    push(right_block, 1, 3, left, 1)
    push(right_block, 1, 5, partner, 1)

    for h in range(2):
        arrive(partner, h, 0, h)
    attend(lambda u: (chip, lax.div(jnp.int32(u), pairs), jnp.int32(u)), chip * 0 + 2 * units, True)

    def seen(c):
        return jnp.where(c < chip, units, 0)

    begin1 = seen(left_chip) + seen(right_chip)
    begin2 = 2 * begin1
    count = begin2 + 2 * seen(far_chip)

    def round0():
        arrive(left_mate, 0, 4, 0)
        arrive(right_mate, 1, 5, 1)

    def round1():
        arrive(left_block, 1, 1, 1)
        push(left_block, 1, 4, partner, 1)
        arrive(right_block, 0, 2, 0)
        push(right_block, 0, 5, partner, 0)
        arrive(left_mate, 1, 4, 1)
        arrive(right_mate, 0, 5, 0)

    def round2():
        for h in range(2):
            arrive(far_block, h, 3, h)
            push(far_block, h, 6, partner, h)
        for h in range(2):
            arrive(far_mate, h, 6, h)

    def where(u):
        turn = jnp.where(u < begin1, 0, jnp.where(u < begin2, 1, 2))
        u = u - jnp.where(turn == 0, 0, jnp.where(turn == 1, begin1, begin2))
        second = lax.div(u, units)
        c = jnp.where(turn == 2, far_chip, jnp.where(second == 0, left_chip, right_chip))
        h = lax.rem(turn + second, 2)
        u = u - second * units
        at = h * units + u
        return c, lax.div(at, pairs), at

    def before(i):
        @pl.when(lax.div(begin1 - 2, 6) == i)
        def _():
            round1()

        @pl.when((lax.div(begin2 - 2, 6) == i) & (begin2 < count))
        def _():
            round2()

    round0()

    @pl.when(count > 0)
    def _():
        attend(where, count, False, before)

    @pl.when(count == 0)
    def _():
        round1()

    @pl.when(begin2 == count)
    def _():
        round2()

    def finish(first, _):
        for i in range(8):
            at = first * 4 + i // 2
            mixed = acc_s[at, :, i % 2 * own : (i % 2 + 1) * own]
            out = (mixed[:HEAD] * (1 / mixed[HEAD : HEAD + 1])).astype(jnp.bfloat16)
            o_s[:, pl.ds(pl.multiple_of((first * 8 + i) * HEAD, HEAD), HEAD)] = out.T
        return _

    lax.fori_loop(0, heads // 8, finish, None)

    def columns(c):
        return pl.ds(pl.multiple_of(c * WIDE, WIDE), WIDE)

    def result(c):
        return pltpu.make_async_copy(x_s.at[:, columns(c)], y_hbm.at[:, columns(c)], y_sem.at[c])

    def add(c):
        x_s[:, columns(c)] = (x_s[:, columns(c)].astype(jnp.float32) + sum_s[...]).astype(jnp.bfloat16)

    def out(c, _):
        for part in range(o_rows):
            fetch_wo(o_rows * c + part).wait()
        last = jnp.maximum(c - 1, 0)
        add(last)
        total = None
        for part in range(o_rows):
            term = _dot(o_s[:, part * DEPTH : (part + 1) * DEPTH], ring[lax.rem(o_first + o_rows * c + part, SLOTS)])
            total = term if total is None else total + term
        sum_s[...] = total

        @pl.when(c < reload)
        def _():
            for part in range(o_rows):
                fetch_wo(o_rows * c + part + SLOTS).start()

        @pl.when(c > 0)
        def _():
            result(last).start()

        return _

    sum_s[...] = jnp.zeros_like(sum_s)
    lax.fori_loop(0, o_chunks, out, None)
    add(o_chunks - 1)
    result(o_chunks - 1).start()
    for c in range(o_chunks):
        result(c).wait()

    for h in range(2):
        for slot in range(7):
            for part in range(2):
                push_part(me, h, slot, partner, h, part).wait_send()


def _copy(a_hbm, b_hbm, held, sem):
    rows = a_hbm.shape[0] // 8
    reads = [pltpu.make_async_copy(a_hbm.at[pl.ds(i * rows, rows)], held.at[pl.ds(i * rows, rows)], sem.at[0, i]) for i in range(8)]
    writes = [pltpu.make_async_copy(held.at[pl.ds(i * rows, rows)], b_hbm.at[pl.ds(i * rows, rows)], sem.at[1, i]) for i in range(8)]
    for read in reads:
        read.start()
    for read, write in zip(reads, writes):
        read.wait()
        write.start()
    for write in writes:
        write.wait()


def solution(mesh):
    n = mesh.shape["sp"]

    def step(x, gain, wq, wk, wv, wo):
        own, d = x.shape
        heads, kv_heads = wq.shape[1] // HEAD, wk.shape[1] // HEAD
        half = HEAD // 2
        rate = np.float32(THETA) ** (-(np.arange(HEAD) % half).astype(np.float32) / half)
        anywhere = pl.BlockSpec(memory_space=pl.ANY)
        bf16, f32 = jnp.bfloat16, jnp.float32
        pairs, span = heads // 2, 2 * own
        y = pl.pallas_call(
            functools.partial(_kernel, n),
            out_shape=jax.ShapeDtypeStruct((own, d), bf16),
            in_specs=[anywhere] * 7,
            out_specs=anywhere,
            scratch_shapes=[
                pltpu.VMEM((own, d), bf16),
                pltpu.VMEM((own, d), bf16),
                pltpu.VMEM((SLOTS, DEPTH, WIDE), bf16),
                pltpu.VMEM((n, 2, kv_heads, own, HEAD), bf16),
                pltpu.VMEM((heads, own, HEAD), bf16),
                pltpu.VMEM((pairs, HEAD + 8, span), f32),
                pltpu.VMEM((pairs, 1, span), f32),
                pltpu.VMEM((own, heads * HEAD), bf16),
                pltpu.VMEM((span, own), f32),
                pltpu.VMEM((own, WIDE), bf16),
                pltpu.VMEM((own, WIDE), f32),
                pltpu.VMEM((span, span), f32),
                pltpu.VMEM((span, span), f32),
                pltpu.VMEM((span, span), bf16),
                pltpu.VMEM((span, span), bf16),
                pltpu.VMEM((1, span), f32),
                pltpu.VMEM((1, span), f32),
                pltpu.VMEM((1, span), f32),
                pltpu.VMEM((1, span), f32),
                pltpu.VMEM((d // HEAD, HEAD), bf16),
                pltpu.VMEM((1, HEAD), f32),
                pltpu.VMEM((own, HEAD), f32),
                pltpu.VMEM((own, HEAD), f32),
                pltpu.SemaphoreType.DMA,
                pltpu.SemaphoreType.DMA((2,)),
                pltpu.SemaphoreType.DMA((wo.shape[1] // WIDE,)),
                pltpu.SemaphoreType.DMA((SLOTS,)),
                pltpu.SemaphoreType.DMA((7, 2, 2)),
                pltpu.SemaphoreType.DMA((7, 2, 2)),
            ],
            compiler_params=pltpu.CompilerParams(collective_id=0, has_side_effects=True, vmem_limit_bytes=67043328),
            cost_estimate=pl.CostEstimate(flops=2 * own * d * (2 * wq.shape[1] + 2 * wk.shape[1]), transcendentals=heads * own * own * n,
                                          bytes_accessed=2 * (2 * wq.size + 2 * wk.size)),
        )(x, gain.reshape(d // HEAD, HEAD), jnp.asarray(rate, f32).reshape(1, HEAD), wq, wk, wv, wo)
        return pl.pallas_call(
            _copy,
            out_shape=jax.ShapeDtypeStruct((own, d), bf16),
            in_specs=[anywhere],
            out_specs=anywhere,
            scratch_shapes=[pltpu.VMEM((own, d), bf16), pltpu.SemaphoreType.DMA((2, 8))],
        )(y)

    tokens, whole = P(("dp", "sp"), None), P(None, None)
    return jax.shard_map(
        step,
        mesh=mesh,
        in_specs=(tokens, P(None), whole, whole, whole, whole),
        out_specs=tokens,
        check_vma=False,
    )
```

```python
import functools

import jax
import jax.numpy as jnp
import numpy as np
from jax import lax
from jax.experimental import pallas as pl
from jax.experimental.pallas import tpu as pltpu
from jax.sharding import PartitionSpec as P

HEAD = 128
THETA = 10000
HIDDEN = -2e30
LOG2E = 1.4426950408889634
DEPTH = 2048
WIDE = 512
SLOTS = 12
MESH = pl.DeviceIdType.MESH


def _dot(a, b, ca=1, cb=0):
    return lax.dot_general(a, b, (((ca,), (cb,)), ((), ())), preferred_element_type=jnp.float32)


def _kernel(n, x_hbm, gain_hbm, rate_hbm, wq, wk, wv, wo, y_hbm, x_s, a_s, ring, kv_s, q_s, acc_s, top_s, o_s, bias_s,
            raw_s, sum_s, s0_s, s1_s, p0_s, p1_s, t0_s, t1_s, r0_s, r1_s, gain_s, rate_s, cos_s, sin_s, x_sem, small_sem, y_sem, ring_sem, send_sem, recv_sem):
    own, d = x_s.shape
    heads, kv_heads = q_s.shape[0], kv_s.shape[2]
    group, half = heads // kv_heads, kv_heads // 2
    per = WIDE // HEAD
    e = HEAD**-0.5 * LOG2E
    me = lax.axis_index("sp")
    chips = n // 2
    core, chip = lax.rem(me, 2), lax.div(me, 2)
    right_chip, left_chip = lax.rem(chip + 1, chips), lax.rem(chip + chips - 1, chips)
    far_chip = lax.rem(chip + 2, chips)
    partner, right, left = chip * 2 + 1 - core, right_chip * 2 + core, left_chip * 2 + core

    rows = d // DEPTH
    o_rows = wo.shape[0] // DEPTH
    kv_chunks = kv_heads // per
    q_chunks, o_chunks = heads // per, wo.shape[1] // WIDE
    q_first = 2 * kv_chunks * rows
    o_first = q_first + q_chunks * rows
    ahead = SLOTS // rows
    reload = o_chunks - SLOTS // o_rows

    def fetch(src, part, chunk, slot):
        slot = slot % SLOTS if isinstance(slot, int) else lax.rem(slot, SLOTS)
        return pltpu.make_async_copy(src.at[pl.ds(part * DEPTH, DEPTH), pl.ds(chunk * WIDE, WIDE)], ring.at[slot], ring_sem.at[slot])

    def fetch_static(slot):
        if slot < q_first:
            c, part = slot // rows, slot % rows
            return fetch((wk, wv)[c % 2], part, c // 2, slot)
        c, part = (slot - q_first) // rows, (slot - q_first) % rows
        return fetch(wq, part, c, slot)

    def fetch_wq(c, part):
        return fetch(wq, part, c, q_first + rows * c + part)

    def fetch_wo(t):
        return fetch(wo, lax.rem(t, o_rows), lax.div(t, o_rows), o_first + t)

    def fetch_range(first, last):
        for slot in range(first, last):
            fetch_static(slot).start()

    x_copy = pltpu.make_async_copy(x_hbm, x_s, x_sem)
    x_copy.start()
    small = [pltpu.make_async_copy(gain_hbm, gain_s, small_sem.at[0]), pltpu.make_async_copy(rate_hbm, rate_s, small_sem.at[1])]
    for copy in small:
        copy.start()
    fetch_range(0, rows)

    barrier = pltpu.get_barrier_semaphore()
    for peer in (partner, right, left):
        pl.semaphore_signal(barrier, inc=1, device_id={"sp": peer}, device_id_type=MESH)

    def push_part(owner, h, slot, to, lane, part):
        ref = kv_s.at[owner, part, pl.ds(h * half, half)]
        return pltpu.make_async_remote_copy(ref, ref, send_sem.at[slot, lane, part], recv_sem.at[slot, lane, part], device_id={"sp": to},
                                            device_id_type=MESH)

    def push(owner, h, slot, to, lane):
        for part in range(2):
            push_part(owner, h, slot, to, lane, part).start()

    left_block, right_block, far_block = left_chip * 2 + core, right_chip * 2 + core, far_chip * 2 + core
    left_mate, right_mate, far_mate = left_chip * 2 + 1 - core, right_chip * 2 + 1 - core, far_chip * 2 + 1 - core

    for copy in small:
        copy.wait()
    angle = (me * own + lax.broadcasted_iota(jnp.int32, (own, HEAD), 0)).astype(jnp.float32) * rate_s[...]
    cos_s[...] = jnp.cos(angle)
    sin_s[...] = jnp.where(lax.broadcasted_iota(jnp.int32, (own, HEAD), 1) < HEAD // 2, -1.0, 1.0) * jnp.sin(angle)
    gain = jnp.concatenate([gain_s[i : i + 1, :].astype(jnp.float32) for i in range(d // HEAD)], axis=1)

    x_copy.wait()
    fetch_range(rows, 4 * rows)

    def norm(i, _):
        at = pl.ds(i * 32, 32)
        wide = x_s[at, :].astype(jnp.float32)
        scale = lax.rsqrt(jnp.mean(wide * wide, -1, keepdims=True) + 1e-6)
        a_s[at, :] = (wide * scale * gain).astype(jnp.bfloat16)
        return _

    lax.fori_loop(0, own // 32, norm, None, unroll=2)
    fetch_range(4 * rows, SLOTS)

    def slot_of(first, part):
        return (first + part) % SLOTS if isinstance(first, int) else lax.rem(first + part, SLOTS)

    def project(first, before):
        for part in range(rows):
            slot = slot_of(first, part)
            pltpu.make_async_copy(wq.at[pl.ds(0, DEPTH), pl.ds(0, WIDE)], ring.at[slot], ring_sem.at[slot]).wait()
        before()
        total = None
        for part in range(rows):
            term = _dot(a_s[:, part * DEPTH : (part + 1) * DEPTH], ring[slot_of(first, part)])
            total = term if total is None else total + term
        raw_s[...] = total.astype(jnp.bfloat16)

    def turned(i):
        t = raw_s[:, i * HEAD : (i + 1) * HEAD].astype(jnp.float32)
        return (t * cos_s[...] + pltpu.roll(t, HEAD // 2, 1) * sin_s[...]).astype(jnp.bfloat16)

    def keys(c):
        for i in range(per):
            kv_s[me, 0, c * per + i] = turned(i)

    def values(c):
        for i in range(per):
            for b in range(own // HEAD):
                kv_s[me, 1, c * per + i, b * HEAD : (b + 1) * HEAD, :] = raw_s[b * HEAD : (b + 1) * HEAD, i * HEAD : (i + 1) * HEAD].T

    def queries(c):
        for i in range(per):
            q_s[c * per + i] = turned(i)

    def kv(c, _):
        @pl.when(c == kv_chunks - 1)
        def _():
            pl.semaphore_wait(barrier, 3)
            push_part(me, 0, 1, right, 0, 0).start()

        project(2 * rows * c, lambda: values(jnp.maximum(c - 1, 0)))
        for part in range(rows):
            fetch_wq(2 * c + ahead - 2 * kv_chunks, part).start()

        @pl.when(c == kv_chunks - 1)
        def _():
            push_part(me, 0, 1, right, 0, 1).start()

        project(2 * rows * c + rows, lambda: keys(c))

        for part in range(rows):
            fetch_wq(2 * c + 1 + ahead - 2 * kv_chunks, part).start()
        return _

    lax.fori_loop(0, kv_chunks, kv, None)
    push_part(me, 1, 2, left, 1, 0).start()
    values(kv_chunks - 1)

    def query(c, _):
        project(q_first + rows * c, lambda: queries(jnp.maximum(c - 1, 0)))

        sends = {
            q_chunks // 4: [(1, 2, left, 1, 1)],
            q_chunks // 4 + 1: [(1, 1, right, 1, 0)],
            q_chunks // 2: [(0, 2, left, 0, 0), (0, 0, partner, 0, 0), (0, 0, partner, 0, 1)],
            q_chunks // 2 + 2: [(1, 1, right, 1, 1), (1, 0, partner, 1, 0), (1, 0, partner, 1, 1)],
            q_chunks - 3: [(0, 2, left, 0, 1)],
        }
        for when, parts in sends.items():

            @pl.when(c == when)
            def _():
                for h, slot, to, lane, part in parts:
                    push_part(me, h, slot, to, lane, part).start()

        @pl.when(c < q_chunks - ahead)
        def _():
            for part in range(rows):
                fetch_wq(c + ahead, part).start()

        @pl.when(c >= q_chunks - ahead)
        def _():
            for part in range(rows):
                fetch_wo(rows * (c + ahead - q_chunks) + part).start()

        return _

    lax.fori_loop(0, q_chunks, query, None)
    queries(q_chunks - 1)

    span = 2 * own
    place = lax.broadcasted_iota(jnp.int32, (span, own), 1) - lax.broadcasted_iota(jnp.int32, (span, own), 0) + core * own
    bias_s[...] = jnp.where(place >= 0, 0.0, HIDDEN)
    pairs = group // 2
    units = half * pairs
    s_s, p_s, t_s, r_s = (s0_s, s1_s), (p0_s, p1_s), (t0_s, t1_s), (r0_s, r1_s)

    def attend(where, count, first, deep, before=None):
        def scores(unit, slot):
            c, g, at = unit
            k = jnp.concatenate([kv_s[2 * c, 0, g], kv_s[2 * c + 1, 0, g]], axis=0)
            s = _dot(k, q_s[pl.ds(2 * at, 2)].reshape(2 * own, HEAD), 1, 1)
            if first:
                s = s + jnp.concatenate([bias_s[...], bias_s[...]], axis=1)
            s_s[slot][...] = s
            top = s.max(axis=0, keepdims=True)
            if not first:
                old = top_s[at]
                top = jnp.maximum(old, top)
                r_s[slot][...] = jnp.exp2((old - top) * e)
            top_s[at] = top
            t_s[slot][...] = top

        def weights(slot):
            for r in range(0, span, span // 8):
                at = slice(r, r + span // 8)
                p_s[slot][at, :] = jnp.exp2((s_s[slot][at, :] - t_s[slot][...]) * e).astype(jnp.bfloat16)

        def mix(unit, slot):
            c, g, at = unit
            squares = [kv_s[2 * c + i, 1, g, b * HEAD : (b + 1) * HEAD, :] for i in range(2) for b in range(own // HEAD)]
            v = jnp.concatenate([jnp.concatenate(squares, axis=1), jnp.ones((8, span), jnp.bfloat16)], axis=0)
            new = _dot(v, p_s[slot][...])
            acc_s[at] = new if first else acc_s[at] * r_s[slot][...] + new

        def body(i, _):
            if before is not None:
                before(i)
            held = [where(deep * i + k) for k in range(deep + 2)]
            for k in range(deep):
                mix(held[k], k % 2)
                scores(held[k + 2], k % 2)
                weights(1 - k % 2)
            return _

        scores(where(0), 0)
        scores(where(1), 1)
        weights(0)
        lax.fori_loop(0, lax.div(count, deep) - 1, body, None)
        for k in range(deep, 2, -1):
            mix(where(count - k), k % 2)
            scores(where(count - k + 2), k % 2)
            weights(1 - k % 2)
        mix(where(count - 2), 0)
        weights(1)
        mix(where(count - 1), 1)

    def arrive(owner, h, slot, lane):
        for part in range(2):
            push_part(owner, h, slot, me, lane, part).wait_recv()

    arrive(left_block, 0, 1, 0)
    push(left_block, 0, 3, right, 0)
    push(left_block, 0, 4, partner, 0)
    arrive(right_block, 1, 2, 1)
    push(right_block, 1, 3, left, 1)
    push(right_block, 1, 5, partner, 1)

    for h in range(2):
        arrive(partner, h, 0, h)
    attend(lambda u: (chip, lax.div(jnp.int32(u), pairs), jnp.int32(u)), chip * 0 + 2 * units, True, units // 2)

    def seen(c):
        return jnp.where(c < chip, units, 0)

    begin1 = seen(left_chip) + seen(right_chip)
    begin2 = 2 * begin1
    count = begin2 + 2 * seen(far_chip)

    def round0():
        arrive(left_mate, 0, 4, 0)
        arrive(right_mate, 1, 5, 1)

    def round1():
        arrive(left_block, 1, 1, 1)
        push(left_block, 1, 4, partner, 1)
        arrive(right_block, 0, 2, 0)
        push(right_block, 0, 5, partner, 0)
        arrive(left_mate, 1, 4, 1)
        arrive(right_mate, 0, 5, 0)

    def round2():
        for h in range(2):
            arrive(far_block, h, 3, h)
            push(far_block, h, 6, partner, h)
        for h in range(2):
            arrive(far_mate, h, 6, h)

    def where(u):
        turn = jnp.where(u < begin1, 0, jnp.where(u < begin2, 1, 2))
        u = u - jnp.where(turn == 0, 0, jnp.where(turn == 1, begin1, begin2))
        second = lax.div(u, units)
        c = jnp.where(turn == 2, far_chip, jnp.where(second == 0, left_chip, right_chip))
        h = lax.rem(turn + second, 2)
        u = u - second * units
        at = h * units + u
        return c, lax.div(at, pairs), at

    def before(i):
        @pl.when(lax.div(begin1 - 2, units) == i)
        def _():
            round1()

        @pl.when((lax.div(begin2 - 2, units) == i) & (begin2 < count))
        def _():
            round2()

    round0()

    @pl.when(count > 0)
    def _():
        attend(where, count, False, units, before)

    @pl.when(count == 0)
    def _():
        round1()

    @pl.when(begin2 == count)
    def _():
        round2()

    def finish(first, _):
        for i in range(8):
            at = first * 4 + i // 2
            mixed = acc_s[at, :, i % 2 * own : (i % 2 + 1) * own]
            out = (mixed[:HEAD] * (1 / mixed[HEAD : HEAD + 1])).astype(jnp.bfloat16)
            o_s[:, pl.ds(pl.multiple_of((first * 8 + i) * HEAD, HEAD), HEAD)] = out.T
        return _

    lax.fori_loop(0, heads // 8, finish, None)

    def columns(c):
        return pl.ds(pl.multiple_of(c * WIDE, WIDE), WIDE)

    def result(c):
        return pltpu.make_async_copy(x_s.at[:, columns(c)], y_hbm.at[:, columns(c)], y_sem.at[c])

    def add(c):
        x_s[:, columns(c)] = (x_s[:, columns(c)].astype(jnp.float32) + sum_s[...]).astype(jnp.bfloat16)

    def out(c, _):
        for part in range(o_rows):
            fetch_wo(o_rows * c + part).wait()
        last = jnp.maximum(c - 1, 0)
        add(last)
        total = None
        for part in range(o_rows):
            term = _dot(o_s[:, part * DEPTH : (part + 1) * DEPTH], ring[lax.rem(o_first + o_rows * c + part, SLOTS)])
            total = term if total is None else total + term
        sum_s[...] = total

        @pl.when(c < reload)
        def _():
            for part in range(o_rows):
                fetch_wo(o_rows * c + part + SLOTS).start()

        @pl.when(c > 0)
        def _():
            result(last).start()

        return _

    sum_s[...] = jnp.zeros_like(sum_s)
    lax.fori_loop(0, o_chunks, out, None)
    add(o_chunks - 1)
    result(o_chunks - 1).start()
    for c in range(o_chunks):
        result(c).wait()

    for h in range(2):
        for slot in range(7):
            for part in range(2):
                push_part(me, h, slot, partner, h, part).wait_send()


def _copy(a_hbm, b_hbm, held, sem):
    rows = a_hbm.shape[0] // 8
    reads = [pltpu.make_async_copy(a_hbm.at[pl.ds(i * rows, rows)], held.at[pl.ds(i * rows, rows)], sem.at[0, i]) for i in range(8)]
    writes = [pltpu.make_async_copy(held.at[pl.ds(i * rows, rows)], b_hbm.at[pl.ds(i * rows, rows)], sem.at[1, i]) for i in range(8)]
    for read in reads:
        read.start()
    for read, write in zip(reads, writes):
        read.wait()
        write.start()
    for write in writes:
        write.wait()


def solution(mesh):
    n = mesh.shape["sp"]

    def step(x, gain, wq, wk, wv, wo):
        own, d = x.shape
        heads, kv_heads = wq.shape[1] // HEAD, wk.shape[1] // HEAD
        half = HEAD // 2
        rate = np.float32(THETA) ** (-(np.arange(HEAD) % half).astype(np.float32) / half)
        anywhere = pl.BlockSpec(memory_space=pl.ANY)
        bf16, f32 = jnp.bfloat16, jnp.float32
        pairs, span = heads // 2, 2 * own
        y = pl.pallas_call(
            functools.partial(_kernel, n),
            out_shape=jax.ShapeDtypeStruct((own, d), bf16),
            in_specs=[anywhere] * 7,
            out_specs=anywhere,
            scratch_shapes=[
                pltpu.VMEM((own, d), bf16),
                pltpu.VMEM((own, d), bf16),
                pltpu.VMEM((SLOTS, DEPTH, WIDE), bf16),
                pltpu.VMEM((n, 2, kv_heads, own, HEAD), bf16),
                pltpu.VMEM((heads, own, HEAD), bf16),
                pltpu.VMEM((pairs, HEAD + 8, span), f32),
                pltpu.VMEM((pairs, 1, span), f32),
                pltpu.VMEM((own, heads * HEAD), bf16),
                pltpu.VMEM((span, own), f32),
                pltpu.VMEM((own, WIDE), bf16),
                pltpu.VMEM((own, WIDE), f32),
                pltpu.VMEM((span, span), f32),
                pltpu.VMEM((span, span), f32),
                pltpu.VMEM((span, span), bf16),
                pltpu.VMEM((span, span), bf16),
                pltpu.VMEM((1, span), f32),
                pltpu.VMEM((1, span), f32),
                pltpu.VMEM((1, span), f32),
                pltpu.VMEM((1, span), f32),
                pltpu.VMEM((d // HEAD, HEAD), bf16),
                pltpu.VMEM((1, HEAD), f32),
                pltpu.VMEM((own, HEAD), f32),
                pltpu.VMEM((own, HEAD), f32),
                pltpu.SemaphoreType.DMA,
                pltpu.SemaphoreType.DMA((2,)),
                pltpu.SemaphoreType.DMA((wo.shape[1] // WIDE,)),
                pltpu.SemaphoreType.DMA((SLOTS,)),
                pltpu.SemaphoreType.DMA((7, 2, 2)),
                pltpu.SemaphoreType.DMA((7, 2, 2)),
            ],
            compiler_params=pltpu.CompilerParams(collective_id=0, has_side_effects=True, vmem_limit_bytes=67043328),
            cost_estimate=pl.CostEstimate(flops=2 * own * d * (2 * wq.shape[1] + 2 * wk.shape[1]), transcendentals=heads * own * own * n,
                                          bytes_accessed=2 * (2 * wq.size + 2 * wk.size)),
        )(x, gain.reshape(d // HEAD, HEAD), jnp.asarray(rate, f32).reshape(1, HEAD), wq, wk, wv, wo)
        return pl.pallas_call(
            _copy,
            out_shape=jax.ShapeDtypeStruct((own, d), bf16),
            in_specs=[anywhere],
            out_specs=anywhere,
            scratch_shapes=[pltpu.VMEM((own, d), bf16), pltpu.SemaphoreType.DMA((2, 8))],
        )(y)

    tokens, whole = P(("dp", "sp"), None), P(None, None)
    return jax.shard_map(
        step,
        mesh=mesh,
        in_specs=(tokens, P(None), whole, whole, whole, whole),
        out_specs=tokens,
        check_vma=False,
    )
```

```python
import functools

import jax
import jax.numpy as jnp
import numpy as np
from jax import lax
from jax.experimental import pallas as pl
from jax.experimental.pallas import tpu as pltpu
from jax.sharding import PartitionSpec as P

HEAD = 128
THETA = 10000
HIDDEN = -2e30
LOG2E = 1.4426950408889634
DEPTH = 2048
WIDE = 512
SLOTS = 12
MESH = pl.DeviceIdType.MESH


def _dot(a, b, ca=1, cb=0):
    return lax.dot_general(a, b, (((ca,), (cb,)), ((), ())), preferred_element_type=jnp.float32)


def _kernel(n, x_hbm, gain_hbm, rate_hbm, wq, wk, wv, wo, y_hbm, x_s, a_s, ring, kv_s, q_s, acc_s, top_s, o_s, bias_s,
            raw_s, sum_s, s0_s, s1_s, p0_s, p1_s, t0_s, t1_s, r0_s, r1_s, gain_s, rate_s, cos_s, sin_s, x_sem, small_sem, y_sem, ring_sem, send_sem, recv_sem):
    own, d = x_s.shape
    heads, kv_heads = q_s.shape[0], kv_s.shape[2]
    group, half = heads // kv_heads, kv_heads // 2
    per = WIDE // HEAD
    e = HEAD**-0.5 * LOG2E
    me = lax.axis_index("sp")
    chips = n // 2
    core, chip = lax.rem(me, 2), lax.div(me, 2)
    right_chip, left_chip = lax.rem(chip + 1, chips), lax.rem(chip + chips - 1, chips)
    far_chip = lax.rem(chip + 2, chips)
    partner, right, left = chip * 2 + 1 - core, right_chip * 2 + core, left_chip * 2 + core

    rows = d // DEPTH
    o_rows = wo.shape[0] // DEPTH
    kv_chunks = kv_heads // per
    q_chunks, o_chunks = heads // per, wo.shape[1] // WIDE
    q_first = 2 * kv_chunks * rows
    o_first = q_first + q_chunks * rows
    ahead = SLOTS // rows
    reload = o_chunks - SLOTS // o_rows

    def fetch(src, part, chunk, slot):
        slot = slot % SLOTS if isinstance(slot, int) else lax.rem(slot, SLOTS)
        return pltpu.make_async_copy(src.at[pl.ds(part * DEPTH, DEPTH), pl.ds(chunk * WIDE, WIDE)], ring.at[slot], ring_sem.at[slot])

    def fetch_static(slot):
        if slot < q_first:
            c, part = slot // rows, slot % rows
            return fetch((wk, wv)[c % 2], part, c // 2, slot)
        c, part = (slot - q_first) // rows, (slot - q_first) % rows
        return fetch(wq, part, c, slot)

    def fetch_wq(c, part):
        return fetch(wq, part, c, q_first + rows * c + part)

    def fetch_wo(t):
        return fetch(wo, lax.rem(t, o_rows), lax.div(t, o_rows), o_first + t)

    def fetch_range(first, last):
        for slot in range(first, last):
            fetch_static(slot).start()

    x_copy = pltpu.make_async_copy(x_hbm, x_s, x_sem)
    x_copy.start()
    small = [pltpu.make_async_copy(gain_hbm, gain_s, small_sem.at[0]), pltpu.make_async_copy(rate_hbm, rate_s, small_sem.at[1])]
    for copy in small:
        copy.start()
    fetch_range(0, rows)

    barrier = pltpu.get_barrier_semaphore()
    for peer in (partner, right, left):
        pl.semaphore_signal(barrier, inc=1, device_id={"sp": peer}, device_id_type=MESH)

    def push_part(owner, h, slot, to, lane, part):
        ref = kv_s.at[owner, part, pl.ds(h * half, half)]
        return pltpu.make_async_remote_copy(ref, ref, send_sem.at[slot, lane, part], recv_sem.at[slot, lane, part], device_id={"sp": to},
                                            device_id_type=MESH)

    def push(owner, h, slot, to, lane):
        for part in range(2):
            push_part(owner, h, slot, to, lane, part).start()

    left_block, right_block, far_block = left_chip * 2 + core, right_chip * 2 + core, far_chip * 2 + core
    left_mate, right_mate, far_mate = left_chip * 2 + 1 - core, right_chip * 2 + 1 - core, far_chip * 2 + 1 - core

    for copy in small:
        copy.wait()
    angle = (me * own + lax.broadcasted_iota(jnp.int32, (own, HEAD), 0)).astype(jnp.float32) * rate_s[...]
    cos_s[...] = jnp.cos(angle)
    sin_s[...] = jnp.where(lax.broadcasted_iota(jnp.int32, (own, HEAD), 1) < HEAD // 2, -1.0, 1.0) * jnp.sin(angle)
    gain = jnp.concatenate([gain_s[i : i + 1, :].astype(jnp.float32) for i in range(d // HEAD)], axis=1)

    x_copy.wait()
    fetch_range(rows, 4 * rows)

    def norm(i, _):
        at = pl.ds(i * 32, 32)
        wide = x_s[at, :].astype(jnp.float32)
        scale = lax.rsqrt(jnp.mean(wide * wide, -1, keepdims=True) + 1e-6)
        a_s[at, :] = (wide * scale * gain).astype(jnp.bfloat16)
        return _

    lax.fori_loop(0, own // 32, norm, None, unroll=2)
    fetch_range(4 * rows, SLOTS)

    def slot_of(first, part):
        return (first + part) % SLOTS if isinstance(first, int) else lax.rem(first + part, SLOTS)

    def project(first, before):
        for part in range(rows):
            slot = slot_of(first, part)
            pltpu.make_async_copy(wq.at[pl.ds(0, DEPTH), pl.ds(0, WIDE)], ring.at[slot], ring_sem.at[slot]).wait()
        before()
        total = None
        for part in range(rows):
            term = _dot(a_s[:, part * DEPTH : (part + 1) * DEPTH], ring[slot_of(first, part)])
            total = term if total is None else total + term
        raw_s[...] = total.astype(jnp.bfloat16)

    def turned(i):
        t = raw_s[:, i * HEAD : (i + 1) * HEAD].astype(jnp.float32)
        return (t * cos_s[...] + pltpu.roll(t, HEAD // 2, 1) * sin_s[...]).astype(jnp.bfloat16)

    def keys(c):
        for i in range(per):
            kv_s[me, 0, c * per + i] = turned(i)

    def values(c):
        for i in range(per):
            for b in range(own // HEAD):
                kv_s[me, 1, c * per + i, b * HEAD : (b + 1) * HEAD, :] = raw_s[b * HEAD : (b + 1) * HEAD, i * HEAD : (i + 1) * HEAD].T

    def queries(c):
        for i in range(per):
            q_s[c * per + i] = turned(i)

    def kv(c, _):
        @pl.when(c == kv_chunks - 1)
        def _():
            pl.semaphore_wait(barrier, 3)
            push_part(me, 0, 1, right, 0, 0).start()

        project(2 * rows * c, lambda: values(jnp.maximum(c - 1, 0)))
        for part in range(rows):
            fetch_wq(2 * c + ahead - 2 * kv_chunks, part).start()

        @pl.when(c == kv_chunks - 1)
        def _():
            push_part(me, 0, 1, right, 0, 1).start()

        project(2 * rows * c + rows, lambda: keys(c))

        for part in range(rows):
            fetch_wq(2 * c + 1 + ahead - 2 * kv_chunks, part).start()
        return _

    lax.fori_loop(0, kv_chunks, kv, None)
    push_part(me, 1, 2, left, 1, 0).start()
    values(kv_chunks - 1)

    def query(c, _):
        project(q_first + rows * c, lambda: queries(jnp.maximum(c - 1, 0)))

        sends = {
            q_chunks // 4: [(1, 2, left, 1, 1)],
            q_chunks // 4 + 1: [(1, 1, right, 1, 0)],
            q_chunks // 2: [(0, 2, left, 0, 0), (0, 0, partner, 0, 0), (0, 0, partner, 0, 1)],
            q_chunks // 2 + 2: [(1, 1, right, 1, 1), (1, 0, partner, 1, 0), (1, 0, partner, 1, 1)],
            q_chunks - 3: [(0, 2, left, 0, 1)],
        }
        for when, parts in sends.items():

            @pl.when(c == when)
            def _():
                for h, slot, to, lane, part in parts:
                    push_part(me, h, slot, to, lane, part).start()

        @pl.when(c < q_chunks - ahead)
        def _():
            for part in range(rows):
                fetch_wq(c + ahead, part).start()

        @pl.when(c >= q_chunks - ahead)
        def _():
            for part in range(rows):
                fetch_wo(rows * (c + ahead - q_chunks) + part).start()

        return _

    lax.fori_loop(0, q_chunks, query, None)
    queries(q_chunks - 1)

    span = 2 * own
    place = lax.broadcasted_iota(jnp.int32, (span, own), 1) - lax.broadcasted_iota(jnp.int32, (span, own), 0) + core * own
    bias_s[...] = jnp.where(place >= 0, 0.0, HIDDEN)
    pairs = group // 2
    units = half * pairs
    s_s, p_s, t_s, r_s = (s0_s, s1_s), (p0_s, p1_s), (t0_s, t1_s), (r0_s, r1_s)

    def attend(where, count, first, deep, before=None):
        def scores(unit, slot):
            c, g, at = unit
            k = jnp.concatenate([kv_s[2 * c, 0, g], kv_s[2 * c + 1, 0, g]], axis=0)
            s = _dot(k, q_s[pl.ds(2 * at, 2)].reshape(2 * own, HEAD), 1, 1)
            if first:
                s = s + jnp.concatenate([bias_s[...], bias_s[...]], axis=1)
            s_s[slot][...] = s
            top = s.max(axis=0, keepdims=True)
            if not first:
                old = top_s[at]
                top = jnp.maximum(old, top)
                r_s[slot][...] = jnp.exp2((old - top) * e)
            top_s[at] = top
            t_s[slot][...] = top

        def weights(slot):
            for r in range(0, span, span // 8):
                at = slice(r, r + span // 8)
                p_s[slot][at, :] = jnp.exp2((s_s[slot][at, :] - t_s[slot][...]) * e).astype(jnp.bfloat16)

        def mix(unit, slot):
            c, g, at = unit
            squares = [kv_s[2 * c + i, 1, g, b * HEAD : (b + 1) * HEAD, :] for i in range(2) for b in range(own // HEAD)]
            v = jnp.concatenate([jnp.concatenate(squares, axis=1), jnp.ones((8, span), jnp.bfloat16)], axis=0)
            new = _dot(v, p_s[slot][...])
            acc_s[at] = new if first else acc_s[at] * r_s[slot][...] + new

        def body(i, _):
            if before is not None:
                before(i)
            held = [where(deep * i + k) for k in range(deep + 2)]
            for k in range(deep):
                mix(held[k], k % 2)
                scores(held[k + 2], k % 2)
                weights(1 - k % 2)
            return _

        scores(where(0), 0)
        scores(where(1), 1)
        weights(0)
        lax.fori_loop(0, lax.div(count, deep) - 1, body, None)
        for k in range(deep, 2, -1):
            mix(where(count - k), k % 2)
            scores(where(count - k + 2), k % 2)
            weights(1 - k % 2)
        mix(where(count - 2), 0)
        weights(1)
        mix(where(count - 1), 1)

    def arrive(owner, h, slot, lane):
        for part in range(2):
            push_part(owner, h, slot, me, lane, part).wait_recv()

    arrive(left_block, 0, 1, 0)
    push(left_block, 0, 3, right, 0)
    push(left_block, 0, 4, partner, 0)
    arrive(right_block, 1, 2, 1)
    push(right_block, 1, 3, left, 1)
    push(right_block, 1, 5, partner, 1)

    for h in range(2):
        arrive(partner, h, 0, h)
    attend(lambda u: (chip, lax.div(jnp.int32(u), pairs), jnp.int32(u)), chip * 0 + 2 * units, True, units)

    def seen(c):
        return jnp.where(c < chip, units, 0)

    begin1 = seen(left_chip) + seen(right_chip)
    begin2 = 2 * begin1
    count = begin2 + 2 * seen(far_chip)

    def round0():
        arrive(left_mate, 0, 4, 0)
        arrive(right_mate, 1, 5, 1)

    def round1():
        arrive(left_block, 1, 1, 1)
        push(left_block, 1, 4, partner, 1)
        arrive(right_block, 0, 2, 0)
        push(right_block, 0, 5, partner, 0)
        arrive(left_mate, 1, 4, 1)
        arrive(right_mate, 0, 5, 0)

    def round2():
        for h in range(2):
            arrive(far_block, h, 3, h)
            push(far_block, h, 6, partner, h)
        for h in range(2):
            arrive(far_mate, h, 6, h)

    def where(u):
        turn = jnp.where(u < begin1, 0, jnp.where(u < begin2, 1, 2))
        u = u - jnp.where(turn == 0, 0, jnp.where(turn == 1, begin1, begin2))
        second = lax.div(u, units)
        c = jnp.where(turn == 2, far_chip, jnp.where(second == 0, left_chip, right_chip))
        h = lax.rem(turn + second, 2)
        u = u - second * units
        at = h * units + u
        return c, lax.div(at, pairs), at

    def before(i):
        @pl.when(lax.div(begin1 - 2, units) == i)
        def _():
            round1()

        @pl.when((lax.div(begin2 - 2, units) == i) & (begin2 < count))
        def _():
            round2()

    round0()

    @pl.when(count > 0)
    def _():
        attend(where, count, False, units, before)

    @pl.when(count == 0)
    def _():
        round1()

    @pl.when(begin2 == count)
    def _():
        round2()

    def finish(first, _):
        for i in range(8):
            at = first * 4 + i // 2
            mixed = acc_s[at, :, i % 2 * own : (i % 2 + 1) * own]
            out = (mixed[:HEAD] * (1 / mixed[HEAD : HEAD + 1])).astype(jnp.bfloat16)
            o_s[:, pl.ds(pl.multiple_of((first * 8 + i) * HEAD, HEAD), HEAD)] = out.T
        return _

    lax.fori_loop(0, heads // 8, finish, None)

    def columns(c):
        return pl.ds(pl.multiple_of(c * WIDE, WIDE), WIDE)

    def result(c):
        return pltpu.make_async_copy(x_s.at[:, columns(c)], y_hbm.at[:, columns(c)], y_sem.at[c])

    def add(c):
        x_s[:, columns(c)] = (x_s[:, columns(c)].astype(jnp.float32) + sum_s[...]).astype(jnp.bfloat16)

    def out(c, _):
        for part in range(o_rows):
            fetch_wo(o_rows * c + part).wait()
        last = jnp.maximum(c - 1, 0)
        add(last)
        total = None
        for part in range(o_rows):
            term = _dot(o_s[:, part * DEPTH : (part + 1) * DEPTH], ring[lax.rem(o_first + o_rows * c + part, SLOTS)])
            total = term if total is None else total + term
        sum_s[...] = total

        @pl.when(c < reload)
        def _():
            for part in range(o_rows):
                fetch_wo(o_rows * c + part + SLOTS).start()

        @pl.when(c > 0)
        def _():
            result(last).start()

        return _

    sum_s[...] = jnp.zeros_like(sum_s)
    lax.fori_loop(0, o_chunks, out, None)
    add(o_chunks - 1)
    result(o_chunks - 1).start()
    for c in range(o_chunks):
        result(c).wait()

    for h in range(2):
        for slot in range(7):
            for part in range(2):
                push_part(me, h, slot, partner, h, part).wait_send()


def _copy(a_hbm, b_hbm, held, sem):
    rows = a_hbm.shape[0] // 8
    reads = [pltpu.make_async_copy(a_hbm.at[pl.ds(i * rows, rows)], held.at[pl.ds(i * rows, rows)], sem.at[0, i]) for i in range(8)]
    writes = [pltpu.make_async_copy(held.at[pl.ds(i * rows, rows)], b_hbm.at[pl.ds(i * rows, rows)], sem.at[1, i]) for i in range(8)]
    for read in reads:
        read.start()
    for read, write in zip(reads, writes):
        read.wait()
        write.start()
    for write in writes:
        write.wait()


def solution(mesh):
    n = mesh.shape["sp"]

    def step(x, gain, wq, wk, wv, wo):
        own, d = x.shape
        heads, kv_heads = wq.shape[1] // HEAD, wk.shape[1] // HEAD
        half = HEAD // 2
        rate = np.float32(THETA) ** (-(np.arange(HEAD) % half).astype(np.float32) / half)
        anywhere = pl.BlockSpec(memory_space=pl.ANY)
        bf16, f32 = jnp.bfloat16, jnp.float32
        pairs, span = heads // 2, 2 * own
        y = pl.pallas_call(
            functools.partial(_kernel, n),
            out_shape=jax.ShapeDtypeStruct((own, d), bf16),
            in_specs=[anywhere] * 7,
            out_specs=anywhere,
            scratch_shapes=[
                pltpu.VMEM((own, d), bf16),
                pltpu.VMEM((own, d), bf16),
                pltpu.VMEM((SLOTS, DEPTH, WIDE), bf16),
                pltpu.VMEM((n, 2, kv_heads, own, HEAD), bf16),
                pltpu.VMEM((heads, own, HEAD), bf16),
                pltpu.VMEM((pairs, HEAD + 8, span), f32),
                pltpu.VMEM((pairs, 1, span), f32),
                pltpu.VMEM((own, heads * HEAD), bf16),
                pltpu.VMEM((span, own), f32),
                pltpu.VMEM((own, WIDE), bf16),
                pltpu.VMEM((own, WIDE), f32),
                pltpu.VMEM((span, span), f32),
                pltpu.VMEM((span, span), f32),
                pltpu.VMEM((span, span), bf16),
                pltpu.VMEM((span, span), bf16),
                pltpu.VMEM((1, span), f32),
                pltpu.VMEM((1, span), f32),
                pltpu.VMEM((1, span), f32),
                pltpu.VMEM((1, span), f32),
                pltpu.VMEM((d // HEAD, HEAD), bf16),
                pltpu.VMEM((1, HEAD), f32),
                pltpu.VMEM((own, HEAD), f32),
                pltpu.VMEM((own, HEAD), f32),
                pltpu.SemaphoreType.DMA,
                pltpu.SemaphoreType.DMA((2,)),
                pltpu.SemaphoreType.DMA((wo.shape[1] // WIDE,)),
                pltpu.SemaphoreType.DMA((SLOTS,)),
                pltpu.SemaphoreType.DMA((7, 2, 2)),
                pltpu.SemaphoreType.DMA((7, 2, 2)),
            ],
            compiler_params=pltpu.CompilerParams(collective_id=0, has_side_effects=True, vmem_limit_bytes=67043328),
            cost_estimate=pl.CostEstimate(flops=2 * own * d * (2 * wq.shape[1] + 2 * wk.shape[1]), transcendentals=heads * own * own * n,
                                          bytes_accessed=2 * (2 * wq.size + 2 * wk.size)),
        )(x, gain.reshape(d // HEAD, HEAD), jnp.asarray(rate, f32).reshape(1, HEAD), wq, wk, wv, wo)
        return pl.pallas_call(
            _copy,
            out_shape=jax.ShapeDtypeStruct((own, d), bf16),
            in_specs=[anywhere],
            out_specs=anywhere,
            scratch_shapes=[pltpu.VMEM((own, d), bf16), pltpu.SemaphoreType.DMA((2, 8))],
        )(y)

    tokens, whole = P(("dp", "sp"), None), P(None, None)
    return jax.shard_map(
        step,
        mesh=mesh,
        in_specs=(tokens, P(None), whole, whole, whole, whole),
        out_specs=tokens,
        check_vma=False,
    )
```
